8 devices in a mesh: dp: 1 (over z), m3: 2 (over y), m2: 2 (over x), m1: 2 (over core).
Axes of the slice: x: 2, y: 2, z: 1, core: 2. Of those that a mesh axis runs over, the one named last changes fastest.
Arguments:
- volume: bfloat16 [128, 128, 128, 32], P('dp', 'm1', 'm2', 'm3')
- fac_one: bfloat16 [128, 128], replicated
- fac_two: bfloat16 [128, 128], replicated
- fac_three: bfloat16 [32, 32], replicated
- diag_scale: float32 [32, 128, 128], P('m2', 'm1')
Outputs:
- output: bfloat16 [128, 32, 128, 128], P(('dp', 'm3'), 'm2', 'm1')
All inputs are finite; a program needn't handle non-finite values.
Results may differ from the reference program's by a relative error of at most 0.00844113.
Values are sent between devices in bfloat16 or wider.
A program may use at most 1 GiB of HBM per device.

```python
import jax
import jax.numpy as jnp
from jax import lax

GRID_ONE = 128
GRID_TWO = 128
GRID_THREE = 32
RHS_PART = 128


def orthonormal(rng_key, mat_order):
    gaussian = jax.random.normal(rng_key, (mat_order, mat_order), jnp.float32)
    ortho_mat = jnp.linalg.qr(gaussian)[0]
    return ortho_mat.astype(jnp.bfloat16)


def setup_inputs(seed: int = 0, part: int = 0) -> dict:
    base_key = jax.random.key(seed)
    key_list = jax.random.split(base_key, 5)
    vol_key = jax.random.fold_in(key_list[0], part)
    volume = jax.random.normal(vol_key, (RHS_PART, GRID_ONE, GRID_TWO, GRID_THREE), jnp.float32).astype(jnp.bfloat16)
    fac_one = orthonormal(key_list[1], GRID_ONE)
    fac_two = orthonormal(key_list[2], GRID_TWO)
    fac_three = orthonormal(key_list[3], GRID_THREE)
    log_diag = jax.random.uniform(key_list[4], (GRID_THREE, GRID_TWO, GRID_ONE), jnp.float32, -1.15, 1.15)
    diag_scale = jnp.exp(log_diag)
    return {"volume": volume, "fac_one": fac_one, "fac_two": fac_two, "fac_three": fac_three, "diag_scale": diag_scale}


def reference(volume, fac_one, fac_two, fac_three, diag_scale):
    one_wide = fac_one.astype(jnp.float32)
    two_wide = fac_two.astype(jnp.float32)
    three_wide = fac_three.astype(jnp.float32)

    def per_rhs(vol_one):
        prod_three = jnp.einsum("abl,kl->abk", vol_one.astype(jnp.float32), three_wide).astype(jnp.bfloat16)
        prod_two = jnp.einsum("abk,jb->akj", prod_three.astype(jnp.float32), two_wide).astype(jnp.bfloat16)
        prod_one = jnp.einsum("akj,ia->kji", prod_two.astype(jnp.float32), one_wide).astype(jnp.bfloat16)
        return (diag_scale * prod_one.astype(jnp.float32)).astype(jnp.bfloat16)

    return lax.map(per_rhs, volume)
```

```python
import functools

import jax
import jax.numpy as jnp
from jax import lax
from jax.experimental import pallas as pl
from jax.experimental.pallas import tpu as pltpu
from jax.sharding import PartitionSpec as P

MESH = pl.DeviceIdType.MESH
F32, BF16 = jnp.float32, jnp.bfloat16

LANES = 128
SG = 8
AG = 16
RING = 4
BSLAB = 32


def butterfly(tiles, lane_step):
    count = len(tiles)
    lane = lax.broadcasted_iota(jnp.int32, tiles[0].shape, tiles[0].ndim - 1)
    dist = count // 2
    while dist >= 1:
        shift = dist * lane_step
        low = (lane & shift) == 0
        fresh = list(tiles)
        for i in range(count):
            if i & dist:
                continue
            j = i + dist
            axis = tiles[i].ndim - 1
            fresh[i] = jnp.where(low, tiles[i], pltpu.roll(tiles[j], shift, axis))
            fresh[j] = jnp.where(low, pltpu.roll(tiles[i], LANES - shift, axis), tiles[j])
        tiles = fresh
        dist //= 2
    return tiles


def iota(shape, axis):
    return lax.broadcasted_iota(jnp.int32, shape, axis)


def one_hot(cond):
    return jnp.where(cond, 1.0, 0.0).astype(BF16)


def dot(a, b):
    return jnp.dot(a, b, preferred_element_type=F32)


def kernel(x_hbm, a1_ref, a2_ref, a3_ref, d_ref, w_hbm,
           slab, grp, yrecv, u3keep, u3send, xrecv, u2keep, u2send, crecv, wst,
           l3_ref, a2p_ref, a1p_ref,
           slab_sem, w_sem, ysend_sem, yrecv_sem, xsend_sem, xrecv_sem, csend_sem, crecv_sem):
    m3, m2, m1 = lax.axis_index("m3"), lax.axis_index("m2"), lax.axis_index("m1")
    n_a, n_b, n_l, _ = x_hbm.shape
    n_ab = n_a // AG
    n_half = n_b // BSLAB
    n_slab = n_ab * n_half
    n_g = grp.shape[0] // 2
    n_t = n_g * n_ab
    n_k = u3keep.shape[1]
    n_j = u2keep.shape[3]

    def slab_copy(i):
        ab, h = i // n_half, i % n_half
        return pltpu.make_async_copy(
            x_hbm.at[pl.ds(ab * AG, AG), pl.ds(h * BSLAB, BSLAB)], slab.at[i % 2], slab_sem.at[i % 2])

    def y_copy(t):
        g, ab = t // n_ab, t % n_ab
        return pltpu.make_async_remote_copy(
            src_ref=grp.at[(1 - m3) * n_g + g, ab], dst_ref=yrecv.at[t],
            send_sem=ysend_sem.at[t], recv_sem=yrecv_sem.at[t],
            device_id={"m3": 1 - m3}, device_id_type=MESH)

    def x_copy(t):
        return pltpu.make_async_remote_copy(
            src_ref=u3send.at[t % RING], dst_ref=xrecv.at[t],
            send_sem=xsend_sem.at[t % RING], recv_sem=xrecv_sem.at[t],
            device_id={"m2": 1 - m2}, device_id_type=MESH)

    def c_copy(t):
        return pltpu.make_async_remote_copy(
            src_ref=u2send.at[t % RING], dst_ref=crecv.at[t],
            send_sem=csend_sem.at[t % RING], recv_sem=crecv_sem.at[t],
            device_id={"m1": 1 - m1}, device_id_type=MESH)

    def w_copy(g):
        return pltpu.make_async_copy(wst.at[g % 2], w_hbm.at[pl.ds(g * SG, SG)], w_sem.at[g % 2])

    slab_copy(0).start()
    slab_copy(1).start()

    barrier = pltpu.get_barrier_semaphore()
    for partner in ({"m3": 1 - m3}, {"m2": 1 - m2}, {"m1": 1 - m1}):
        pl.semaphore_signal(barrier, inc=1, device_id=partner, device_id_type=MESH)
    pl.semaphore_wait(barrier, 3)

    k_all, l_all = a3_ref.shape
    rows = k_all * 8
    cols = 2 * 8 * n_l
    r, c = iota((rows, k_all), 0), iota((rows, k_all), 1)
    pick_k = one_hot((r // 8 + m2 * n_k) % k_all == c)
    r, c = iota((l_all, cols), 0), iota((l_all, cols), 1)
    pick_l = one_hot((c // (8 * n_l) + m3) % 2 * n_l + c % n_l == r)
    wide = dot(dot(pick_k, a3_ref[...]).astype(BF16), pick_l)
    r, c = iota((rows, cols), 0), iota((rows, cols), 1)
    l3_ref[...] = jnp.where(r % 8 == c // n_l % 8, wide, 0.0).astype(BF16)

    size = a2_ref.shape[0]
    r, c = iota((size, size), 0), iota((size, size), 1)
    pick_j = one_hot((r + m1 * n_j) % size == c)
    pick_b = one_hot((c + m2 * n_b) % size == r)
    a2p_ref[...] = dot(dot(pick_j, a2_ref[...]).astype(BF16), pick_b).astype(BF16)
    v = r % (2 * n_ab)
    pick_a = one_hot((v // n_ab + m1) % 2 * n_a + v % n_ab * AG + r // (2 * n_ab) == c)
    a1p_ref[...] = lax.dot_general(pick_a, a1_ref[...], (((1,), (1,)), ((), ())),
                                   preferred_element_type=F32).astype(BF16)

    def regroup(i, carry):
        ab, h = i // n_half, i % n_half
        slab_copy(i).wait()

        def one_b(b, carry):
            tiles = butterfly([slab[i % 2, a, b] for a in range(AG)], SG)
            for g in range(2 * n_g):
                grp[g, ab, h * BSLAB + b] = tiles[g]
            return carry

        lax.fori_loop(0, BSLAB, one_b, 0)

        @pl.when(i + 2 < n_slab)
        def _():
            slab_copy(i + 2).start()

        @pl.when(h == n_half - 1)
        def _():
            y_copy(ab).start()
        return carry

    lax.fori_loop(0, n_slab, regroup, 0)

    def mode_three(t):
        g, ab = t // n_ab, t % n_ab
        slot = t % RING
        mine = m3 * n_g + g

        def body(bp, carry):
            b0 = bp * 16
            parts = []
            for h in range(2):
                own = grp[mine, ab, pl.ds(b0 + 8 * h, 8)].reshape(8 * n_l, LANES)
                got = yrecv[t, pl.ds(b0 + 8 * h, 8)].reshape(8 * n_l, LANES)
                parts.append(jnp.concatenate([own, got], axis=0))
            out = dot(l3_ref[...], jnp.concatenate(parts, axis=1))
            lo = out[:, :LANES].reshape(2 * n_k, 8, LANES)
            hi = out[:, LANES:].reshape(2 * n_k, 8, LANES)
            full = jnp.concatenate([lo, hi], axis=1).astype(BF16)
            u3keep[slot, :, pl.ds(b0, 16), :] = full[:n_k]
            u3send[slot, :, pl.ds(b0, 16), :] = full[n_k:]
            return carry

        lax.fori_loop(0, n_b // 16, body, 0)

    def mode_two(t):
        g, ab = t // n_ab, t % n_ab
        slot = t % RING

        def body(kp, carry):
            parts = []
            for h in range(2):
                parts.append(jnp.concatenate([u3keep[slot, 2 * kp + h], xrecv[t, 2 * kp + h]], axis=0))
            out = dot(a2p_ref[...], jnp.concatenate(parts, axis=1)).astype(BF16)
            for h in range(2):
                half = out[:, h * LANES:(h + 1) * LANES]
                u2keep[g % 2, ab, 2 * kp + h] = half[:n_j]
                u2send[slot, 2 * kp + h] = half[n_j:]
            return carry

        lax.fori_loop(0, n_k // 2, body, 0)

    def mode_one(g):
        def body(i, carry):
            k, j0 = i // (n_j // 16), i % (n_j // 16) * 16
            tiles = [u2keep[g % 2, ab, k, pl.ds(j0, 16)] for ab in range(n_ab)]
            tiles += [crecv[g * n_ab + ab, k, pl.ds(j0, 16)] for ab in range(n_ab)]
            tiles = butterfly(tiles, 1)
            out = dot(jnp.concatenate(tiles, axis=0), a1p_ref[...]).astype(BF16).astype(F32)
            scale = d_ref[k, pl.ds(j0, 16), :]
            out = (out.reshape(SG, 16, LANES) * scale[None]).astype(BF16)
            wst[g % 2, :, k, pl.ds(j0, 16), :] = out
            return carry

        lax.fori_loop(0, n_k * (n_j // 16), body, 0)

    def step(t, carry):
        @pl.when(t + n_ab < n_t)
        def _():
            y_copy(t + n_ab).start()

        @pl.when(t < n_t)
        def _():
            y_copy(t).wait_recv()

            @pl.when(t >= RING)
            def _():
                x_copy(t - RING).wait_send()
            mode_three(t)
            x_copy(t).start()

        u = t - 1

        @pl.when((u >= 0) & (u < n_t))
        def _():
            x_copy(u).wait_recv()

            @pl.when(u >= RING)
            def _():
                c_copy(u - RING).wait_send()
            mode_two(u)
            c_copy(u).start()

        z = t - 2

        @pl.when((z >= 0) & (z % n_ab == n_ab - 1))
        def _():
            g = z // n_ab

            def wait_core(ab, carry):
                c_copy(g * n_ab + ab).wait_recv()
                return carry
            lax.fori_loop(0, n_ab, wait_core, 0)

            @pl.when(g >= 2)
            def _():
                w_copy(g - 2).wait()
            mode_one(g)
            w_copy(g).start()
        return carry

    lax.fori_loop(0, n_t + 2, step, 0)

    def drain_y(t, carry):
        y_copy(t).wait_send()
        return carry
    lax.fori_loop(0, n_t, drain_y, 0)

    def drain(t, carry):
        x_copy(t).wait_send()
        c_copy(t).wait_send()
        return carry
    lax.fori_loop(n_t - RING, n_t, drain, 0)
    w_copy(n_g - 2).wait()
    w_copy(n_g - 1).wait()


def solution(mesh):
    def local_step(vol_blk, fac_one, fac_two, fac_three, diag_blk):
        n_s, n_a, n_b, n_l = vol_blk.shape
        n_k, n_j, n_i = diag_blk.shape
        x = jnp.transpose(vol_blk, (1, 2, 3, 0))
        n_g = n_s // SG // 2
        n_ab = n_a // AG
        n_t = n_g * n_ab
        vmem = pl.BlockSpec(memory_space=pltpu.VMEM)
        dma = pltpu.SemaphoreType.DMA
        return pl.pallas_call(
            kernel,
            out_shape=jax.ShapeDtypeStruct((n_s // 2, n_k, n_j, n_i), BF16),
            in_specs=[pl.BlockSpec(memory_space=pl.ANY), vmem, vmem, vmem, vmem],
            out_specs=pl.BlockSpec(memory_space=pl.ANY),
            scratch_shapes=[
                pltpu.VMEM((2, AG, BSLAB, n_l, LANES), BF16),
                pltpu.VMEM((2 * n_g, n_ab, n_b, n_l, LANES), BF16),
                pltpu.VMEM((n_t, n_b, n_l, LANES), BF16),
                pltpu.VMEM((RING, n_k, n_b, LANES), BF16),
                pltpu.VMEM((RING, n_k, n_b, LANES), BF16),
                pltpu.VMEM((n_t, n_k, n_b, LANES), BF16),
                pltpu.VMEM((2, n_ab, n_k, n_j, LANES), BF16),
                pltpu.VMEM((RING, n_k, n_j, LANES), BF16),
                pltpu.VMEM((n_t, n_k, n_j, LANES), BF16),
                pltpu.VMEM((2, SG, n_k, n_j, n_i), BF16),
                pltpu.VMEM((fac_three.shape[0] * 8, 2 * 8 * n_l), BF16),
                pltpu.VMEM(fac_two.shape, BF16),
                pltpu.VMEM(fac_one.shape, BF16),
                dma((2,)), dma((2,)),
                dma((n_t,)), dma((n_t,)),
                dma((RING,)), dma((n_t,)),
                dma((RING,)), dma((n_t,)),
            ],
            compiler_params=pltpu.CompilerParams(
                collective_id=0, has_side_effects=True, vmem_limit_bytes=66 * 1024 * 1024 - 4 * 1024 * 1024),
        )(x, fac_one, fac_two, fac_three, diag_blk)

    return jax.shard_map(local_step, mesh=mesh, in_specs=(P("dp", "m1", "m2", "m3"), P(), P(), P(), P("m2", "m1", None)), out_specs=P(("dp", "m3"), "m2", "m1", None), check_vma=False)
```

```python
import functools

import jax
import jax.numpy as jnp
from jax import lax
from jax.experimental import pallas as pl
from jax.experimental.pallas import tpu as pltpu
from jax.sharding import PartitionSpec as P

MESH = pl.DeviceIdType.MESH
F32, BF16 = jnp.float32, jnp.bfloat16

LANES = 128
SG = 8
AG = 16
RING = 4
PB = 16
U2_RING = 3
PAIRED = 2


def butterfly(tiles, lane_step):
    count = len(tiles)
    lane = lax.broadcasted_iota(jnp.int32, tiles[0].shape, tiles[0].ndim - 1)
    dist = count // 2
    while dist >= 1:
        shift = dist * lane_step
        low = (lane & shift) == 0
        fresh = list(tiles)
        for i in range(count):
            if i & dist:
                continue
            j = i + dist
            axis = tiles[i].ndim - 1
            fresh[i] = jnp.where(low, tiles[i], pltpu.roll(tiles[j], shift, axis))
            fresh[j] = jnp.where(low, pltpu.roll(tiles[i], LANES - shift, axis), tiles[j])
        tiles = fresh
        dist //= 2
    return tiles


def iota(shape, axis):
    return lax.broadcasted_iota(jnp.int32, shape, axis)


def one_hot(cond):
    return jnp.where(cond, 1.0, 0.0).astype(BF16)


def dot(a, b):
    return jnp.dot(a, b, preferred_element_type=F32)


def kernel(x_hbm, a1_ref, a2_ref, a3_ref, d_ref, w_hbm,
           slab, grp, yrecv, u3keep, u3send, xrecv, u2keep, u2send, crecv, wst,
           l3_ref, a2p_ref, a1p_ref,
           slab_sem, w_sem, ysend_sem, yrecv_sem, xsend_sem, xrecv_sem, csend_sem, crecv_sem):
    m3, m2, m1 = lax.axis_index("m3"), lax.axis_index("m2"), lax.axis_index("m1")
    n_a, n_b, n_l, _ = x_hbm.shape
    n_ab = n_a // AG
    n_p = n_b // PB
    n_slab = n_ab * n_p
    n_g = grp.shape[0] // 2
    n_t = n_g * n_ab
    n_k = xrecv.shape[2]
    n_j = u2keep.shape[3]
    k_part = n_k // n_ab
    ahead = n_p - 1

    def place(t):
        early = t < PAIRED * n_ab
        return (jnp.where(early, t % PAIRED, t // n_ab), jnp.where(early, t // PAIRED, t % n_ab))

    def index(g, ab):
        return jnp.where(g < PAIRED, ab * PAIRED + g, g * n_ab + ab)

    def slab_copy(i):
        return pltpu.make_async_copy(
            x_hbm.at[pl.ds(i // n_p * AG, AG), pl.ds(i % n_p * PB, PB)], slab.at[i % RING], slab_sem.at[i % RING])

    def y_copy(t, p):
        g, ab = place(t)
        return pltpu.make_async_remote_copy(
            src_ref=grp.at[(1 - m3) * n_g + g, ab, pl.ds(p * PB, PB)], dst_ref=yrecv.at[t, pl.ds(p * PB, PB)],
            send_sem=ysend_sem.at[t * n_p + p], recv_sem=yrecv_sem.at[t * n_p + p],
            device_id={"m3": 1 - m3}, device_id_type=MESH)

    def x_copy(t, p):
        return pltpu.make_async_remote_copy(
            src_ref=u3send.at[t % RING, p], dst_ref=xrecv.at[t, p],
            send_sem=xsend_sem.at[t % RING * n_p + p], recv_sem=xrecv_sem.at[t * n_p + p],
            device_id={"m2": 1 - m2}, device_id_type=MESH)

    def c_copy(t):
        return pltpu.make_async_remote_copy(
            src_ref=u2send.at[t % RING], dst_ref=crecv.at[t],
            send_sem=csend_sem.at[t % RING], recv_sem=crecv_sem.at[t],
            device_id={"m1": 1 - m1}, device_id_type=MESH)

    def w_copy(n):
        g, part = place(n)
        return pltpu.make_async_copy(
            wst.at[n % RING], w_hbm.at[pl.ds(g * SG, SG), pl.ds(part * k_part, k_part)], w_sem.at[n % RING])

    def each(count, do):
        def body(i, carry):
            do(i)
            return carry
        lax.fori_loop(0, count, body, 0)

    for i in range(RING):
        slab_copy(i).start()

    barrier = pltpu.get_barrier_semaphore()
    for partner in ({"m3": 1 - m3}, {"m2": 1 - m2}, {"m1": 1 - m1}):
        pl.semaphore_signal(barrier, inc=1, device_id=partner, device_id_type=MESH)
    pl.semaphore_wait(barrier, 3)

    def regroup(i):
        ab, p = i // n_p, i % n_p
        slab_copy(i).wait()

        def one_b(b, carry):
            tiles = butterfly([slab[i % RING, a, b] for a in range(AG)], SG)
            for g in range(2 * n_g):
                grp[g, ab, p * PB + b] = tiles[g]
            return carry

        lax.fori_loop(0, PB, one_b, 0, unroll=4)

        @pl.when(i + RING < n_slab)
        def _():
            slab_copy(i + RING).start()

        y_copy(ab * PAIRED, p).start()

        @pl.when(p == n_p - 1)
        def _():
            for e in range(1, PAIRED):
                each(n_p, lambda q: y_copy(ab * PAIRED + e, q).start())

    each(ahead, regroup)

    k_all, l_all = a3_ref.shape
    rows = k_all * 8
    cols = 2 * 8 * n_l
    r, c = iota((rows, k_all), 0), iota((rows, k_all), 1)
    pick_k = one_hot((r // 8 + m2 * n_k) % k_all == c)
    r, c = iota((l_all, cols), 0), iota((l_all, cols), 1)
    pick_l = one_hot((c // (8 * n_l) + m3) % 2 * n_l + c % n_l == r)
    wide = dot(dot(pick_k, a3_ref[...]).astype(BF16), pick_l)
    r, c = iota((rows, cols), 0), iota((rows, cols), 1)
    l3_ref[...] = jnp.where(r % 8 == c // n_l % 8, wide, 0.0).astype(BF16)

    size = a2_ref.shape[0]
    r, c = iota((size, size), 0), iota((size, size), 1)
    pick_j = one_hot((r + m1 * n_j) % size == c)
    pick_b = one_hot((c + m2 * n_b) % size == r)
    a2p_ref[...] = dot(dot(pick_j, a2_ref[...]).astype(BF16), pick_b).astype(BF16)
    v = r % (2 * n_ab)
    pick_a = one_hot((v // n_ab + m1) % 2 * n_a + v % n_ab * AG + r // (2 * n_ab) == c)
    a1p_ref[...] = lax.dot_general(pick_a, a1_ref[...], (((1,), (1,)), ((), ())),
                                   preferred_element_type=F32).astype(BF16)

    def mode_three(t, p):
        g, ab = place(t)
        mine = m3 * n_g + g
        parts = []
        for h in range(2):
            b0 = p * PB + 8 * h
            own = grp[mine, ab, pl.ds(b0, 8)].reshape(8 * n_l, LANES)
            got = yrecv[t, pl.ds(b0, 8)].reshape(8 * n_l, LANES)
            parts.append(jnp.concatenate([own, got], axis=0))
        out = dot(l3_ref[...], jnp.concatenate(parts, axis=1))
        lo = out[:, :LANES].reshape(2 * n_k, 8, LANES)
        hi = out[:, LANES:].reshape(2 * n_k, 8, LANES)
        full = jnp.concatenate([lo, hi], axis=1).astype(BF16)
        u3send[t % RING, p] = full[n_k:]
        u3keep[t % 2, p] = full[:n_k]

    def mode_two(t):
        g, ab = place(t)

        def body(kp, carry):
            parts = []
            for k in (2 * kp, 2 * kp + 1):
                parts.append(jnp.concatenate([u3keep[t % 2, p, k] for p in range(n_p)]
                                             + [xrecv[t, p, k] for p in range(n_p)], axis=0))
            out = dot(a2p_ref[...], jnp.concatenate(parts, axis=1)).astype(BF16)
            for h in range(2):
                half = out[:, h * LANES:(h + 1) * LANES]
                u2send[t % RING, 2 * kp + h] = half[n_j:]
                u2keep[g % U2_RING, ab, 2 * kp + h] = half[:n_j]
            return carry

        lax.fori_loop(0, n_k // 2, body, 0, unroll=n_k // 2)

    def mode_one(n):
        g, part = place(n)

        @pl.when(n >= RING)
        def _():
            w_copy(n - RING).wait()

        def body(i, carry):
            k, j0 = i // (n_j // 16), i % (n_j // 16) * 16
            kk = part * k_part + k
            tiles = [u2keep[g % U2_RING, ab, kk, pl.ds(j0, 16)] for ab in range(n_ab)]
            tiles += [crecv[index(g, ab), kk, pl.ds(j0, 16)] for ab in range(n_ab)]
            tiles = butterfly(tiles, 1)
            out = dot(jnp.concatenate(tiles, axis=0), a1p_ref[...]).astype(BF16).astype(F32)
            scale = d_ref[kk, pl.ds(j0, 16), :]
            out = (out.reshape(SG, 16, LANES) * scale[None]).astype(BF16)
            wst[n % RING, :, k, pl.ds(j0, 16), :] = out
            return carry

        lax.fori_loop(0, k_part * (n_j // 16), body, 0, unroll=8)
        w_copy(n).start()

    def wait_core(g):
        each(n_ab, lambda ab: c_copy(index(g, ab)).wait_recv())

    first = PAIRED * n_ab + 1

    def step(t, carry):
        @pl.when((t + 3 >= PAIRED * n_ab) & (t + 3 < n_t))
        def _():
            each(n_p, lambda p: y_copy(t + 3, p).start())

        def piece(p, carry):
            @pl.when(t < n_t)
            def _():
                y_copy(t, p).wait_recv()

                @pl.when(t >= RING)
                def _():
                    x_copy(t - RING, p).wait_send()
                mode_three(t, p)
                x_copy(t, p).start()

                extra = ahead * (t + 1) + p

                @pl.when((p < ahead) & (extra < n_slab))
                def _():
                    regroup(extra)
            return carry

        lax.fori_loop(0, n_p, piece, 0)

        u = t - 1

        @pl.when(u >= 0)
        def _():
            each(n_p, lambda p: x_copy(u, p).wait_recv())

            @pl.when(u >= RING)
            def _():
                c_copy(u - RING).wait_send()
            mode_two(u)
            c_copy(u).start()

        z = t - first

        @pl.when((z >= 0) & (z < n_ab))
        def _():
            @pl.when(z == 0)
            def _():
                each(PAIRED, wait_core)
            each(PAIRED, lambda e: mode_one(z * PAIRED + e))

        @pl.when(z >= n_ab)
        def _():
            n = z - n_ab + PAIRED * n_ab

            @pl.when(z % n_ab == 0)
            def _():
                wait_core(n // n_ab)
            mode_one(n)
        return carry

    lax.fori_loop(0, n_t + 1, step, 0)

    wait_core(n_g - 1)
    each(n_ab, lambda i: mode_one(n_t - n_ab + i))

    def drain_y(t):
        each(n_p, lambda p: y_copy(t, p).wait_send())
    each(n_t, drain_y)

    def drain(i):
        t = n_t - RING + i
        each(n_p, lambda p: x_copy(t, p).wait_send())
        c_copy(t).wait_send()
        w_copy(t).wait()
    each(RING, drain)


def solution(mesh):
    def local_step(vol_blk, fac_one, fac_two, fac_three, diag_blk):
        n_s, n_a, n_b, n_l = vol_blk.shape
        n_k, n_j, n_i = diag_blk.shape
        x = jnp.transpose(vol_blk, (1, 2, 3, 0))
        n_g = n_s // SG // 2
        n_ab = n_a // AG
        n_t = n_g * n_ab
        n_p = n_b // PB
        vmem = pl.BlockSpec(memory_space=pltpu.VMEM)
        dma = pltpu.SemaphoreType.DMA
        return pl.pallas_call(
            kernel,
            out_shape=jax.ShapeDtypeStruct((n_s // 2, n_k, n_j, n_i), BF16),
            in_specs=[pl.BlockSpec(memory_space=pl.ANY), vmem, vmem, vmem, vmem],
            out_specs=pl.BlockSpec(memory_space=pl.ANY),
            scratch_shapes=[
                pltpu.VMEM((RING, AG, PB, n_l, LANES), BF16),
                pltpu.VMEM((2 * n_g, n_ab, n_b, n_l, LANES), BF16),
                pltpu.VMEM((n_t, n_b, n_l, LANES), BF16),
                pltpu.VMEM((2, n_p, n_k, PB, LANES), BF16),
                pltpu.VMEM((RING, n_p, n_k, PB, LANES), BF16),
                pltpu.VMEM((n_t, n_p, n_k, PB, LANES), BF16),
                pltpu.VMEM((U2_RING, n_ab, n_k, n_j, LANES), BF16),
                pltpu.VMEM((RING, n_k, n_j, LANES), BF16),
                pltpu.VMEM((n_t, n_k, n_j, LANES), BF16),
                pltpu.VMEM((RING, SG, n_k // n_ab, n_j, n_i), BF16),
                pltpu.VMEM((fac_three.shape[0] * 8, 2 * 8 * n_l), BF16),
                pltpu.VMEM(fac_two.shape, BF16),
                pltpu.VMEM(fac_one.shape, BF16),
                dma((RING,)), dma((RING,)),
                dma((n_t * n_p,)), dma((n_t * n_p,)),
                dma((RING * n_p,)), dma((n_t * n_p,)),
                dma((RING,)), dma((n_t,)),
            ],
            compiler_params=pltpu.CompilerParams(
                collective_id=0, has_side_effects=True, vmem_limit_bytes=62 * 1024 * 1024),
        )(x, fac_one, fac_two, fac_three, diag_blk)

    return jax.shard_map(local_step, mesh=mesh, in_specs=(P("dp", "m1", "m2", "m3"), P(), P(), P(), P("m2", "m1", None)), out_specs=P(("dp", "m3"), "m2", "m1", None), check_vma=False)
```

```python
import functools

import jax
import jax.numpy as jnp
from jax import lax
from jax.experimental import pallas as pl
from jax.experimental.pallas import tpu as pltpu
from jax.sharding import PartitionSpec as P

MESH = pl.DeviceIdType.MESH
F32, BF16 = jnp.float32, jnp.bfloat16

LANES = 128
SG = 8
AG = 16
RING = 4
PB = 16
U2_RING = 3
PAIRED = 2


def butterfly(tiles, lane_step):
    count = len(tiles)
    lane = lax.broadcasted_iota(jnp.int32, tiles[0].shape, tiles[0].ndim - 1)
    dist = count // 2
    while dist >= 1:
        shift = dist * lane_step
        low = (lane & shift) == 0
        fresh = list(tiles)
        for i in range(count):
            if i & dist:
                continue
            j = i + dist
            axis = tiles[i].ndim - 1
            fresh[i] = jnp.where(low, tiles[i], pltpu.roll(tiles[j], shift, axis))
            fresh[j] = jnp.where(low, pltpu.roll(tiles[i], LANES - shift, axis), tiles[j])
        tiles = fresh
        dist //= 2
    return tiles


def iota(shape, axis):
    return lax.broadcasted_iota(jnp.int32, shape, axis)


def one_hot(cond):
    return jnp.where(cond, 1.0, 0.0).astype(BF16)


def dot(a, b):
    return jnp.dot(a, b, preferred_element_type=F32)


def kernel(x_hbm, a1_ref, a2_ref, a3_ref, d_ref, w_ref,
           slab, grp, yrecv, u3keep, u3send, xrecv, u2keep, u2send, crecv,
           l3_ref, a2p_ref, a1p_ref,
           slab_sem, free_sem, ysend_sem, yrecv_sem, xsend_sem, xrecv_sem, csend_sem, crecv_sem):
    m3, m2, m1 = lax.axis_index("m3"), lax.axis_index("m2"), lax.axis_index("m1")
    n_a, n_b, n_l, _ = x_hbm.shape
    n_ab = n_a // AG
    n_p = n_b // PB
    n_slab = n_ab * n_p
    n_g = grp.shape[0] // 2
    n_t = n_g * n_ab
    n_k = xrecv.shape[2]
    n_j = u2keep.shape[3]
    k_part = n_k // n_ab
    ahead = n_p - 1

    def place(t):
        early = t < PAIRED * n_ab
        return (jnp.where(early, t % PAIRED, t // n_ab), jnp.where(early, t // PAIRED, t % n_ab))

    def index(g, ab):
        return jnp.where(g < PAIRED, ab * PAIRED + g, g * n_ab + ab)

    def slab_copy(i):
        return pltpu.make_async_copy(
            x_hbm.at[pl.ds(i // n_p * AG, AG), pl.ds(i % n_p * PB, PB)], slab.at[i % RING], slab_sem.at[i % RING])

    def y_copy(t, p):
        g, ab = place(t)
        return pltpu.make_async_remote_copy(
            src_ref=grp.at[(1 - m3) * n_g + g, ab, pl.ds(p * PB, PB)], dst_ref=yrecv.at[t, pl.ds(p * PB, PB)],
            send_sem=ysend_sem.at[t * n_p + p], recv_sem=yrecv_sem.at[t * n_p + p],
            device_id={"m3": 1 - m3}, device_id_type=MESH)

    def x_copy(t, p):
        return pltpu.make_async_remote_copy(
            src_ref=u3send.at[t % RING, p], dst_ref=xrecv.at[t, p],
            send_sem=xsend_sem.at[t % RING * n_p + p], recv_sem=xrecv_sem.at[t * n_p + p],
            device_id={"m2": 1 - m2}, device_id_type=MESH)

    def room(t):
        g, ab = place(t)
        return g % U2_RING * n_ab + ab

    def c_copy(t):
        return pltpu.make_async_remote_copy(
            src_ref=u2send.at[t % RING], dst_ref=crecv.at[room(t)],
            send_sem=csend_sem.at[t % RING], recv_sem=crecv_sem.at[t],
            device_id={"m1": 1 - m1}, device_id_type=MESH)

    def each(count, do):
        def body(i, carry):
            do(i)
            return carry
        lax.fori_loop(0, count, body, 0)

    for i in range(RING):
        slab_copy(i).start()

    barrier = pltpu.get_barrier_semaphore()
    for partner in ({"m3": 1 - m3}, {"m2": 1 - m2}, {"m1": 1 - m1}):
        pl.semaphore_signal(barrier, inc=1, device_id=partner, device_id_type=MESH)
    pl.semaphore_wait(barrier, 3)

    def regroup(i):
        ab, p = i // n_p, i % n_p
        slab_copy(i).wait()

        def one_b(b, carry):
            tiles = butterfly([slab[i % RING, a, b] for a in range(AG)], SG)
            for g in range(2 * n_g):
                grp[g, ab, p * PB + b] = tiles[g]
            return carry

        lax.fori_loop(0, PB, one_b, 0, unroll=4)

        @pl.when(i + RING < n_slab)
        def _():
            slab_copy(i + RING).start()

        y_copy(ab * PAIRED, p).start()

        @pl.when(p == n_p - 1)
        def _():
            for e in range(1, PAIRED):
                each(n_p, lambda q: y_copy(ab * PAIRED + e, q).start())

    each(ahead, regroup)

    k_all, l_all = a3_ref.shape
    rows = k_all * 8
    cols = 2 * 8 * n_l
    r, c = iota((rows, k_all), 0), iota((rows, k_all), 1)
    pick_k = one_hot((r // 8 + m2 * n_k) % k_all == c)
    r, c = iota((l_all, cols), 0), iota((l_all, cols), 1)
    pick_l = one_hot((c // (8 * n_l) + m3) % 2 * n_l + c % n_l == r)
    wide = dot(dot(pick_k, a3_ref[...]).astype(BF16), pick_l)
    r, c = iota((rows, cols), 0), iota((rows, cols), 1)
    l3_ref[...] = jnp.where(r % 8 == c // n_l % 8, wide, 0.0).astype(BF16)

    size = a2_ref.shape[0]
    r, c = iota((size, size), 0), iota((size, size), 1)
    pick_j = one_hot((r + m1 * n_j) % size == c)
    pick_b = one_hot((c + m2 * n_b) % size == r)
    a2p_ref[...] = dot(dot(pick_j, a2_ref[...]).astype(BF16), pick_b).astype(BF16)
    v = r % (2 * n_ab)
    pick_a = one_hot((v // n_ab + m1) % 2 * n_a + v % n_ab * AG + r // (2 * n_ab) == c)
    a1p_ref[...] = lax.dot_general(pick_a, a1_ref[...], (((1,), (1,)), ((), ())),
                                   preferred_element_type=F32).astype(BF16)

    def mode_three(t, p):
        g, ab = place(t)
        mine = m3 * n_g + g
        parts = []
        for h in range(2):
            b0 = p * PB + 8 * h
            own = grp[mine, ab, pl.ds(b0, 8)].reshape(8 * n_l, LANES)
            got = yrecv[t, pl.ds(b0, 8)].reshape(8 * n_l, LANES)
            parts.append(jnp.concatenate([own, got], axis=0))
        out = dot(l3_ref[...], jnp.concatenate(parts, axis=1))
        lo = out[:, :LANES].reshape(2 * n_k, 8, LANES)
        hi = out[:, LANES:].reshape(2 * n_k, 8, LANES)
        full = jnp.concatenate([lo, hi], axis=1).astype(BF16)
        u3send[t % RING, p] = full[n_k:]
        u3keep[t % 2, p] = full[:n_k]

    def mode_two(t):
        g, ab = place(t)

        def body(kp, carry):
            parts = []
            for k in (2 * kp, 2 * kp + 1):
                parts.append(jnp.concatenate([u3keep[t % 2, p, k] for p in range(n_p)]
                                             + [xrecv[t, p, k] for p in range(n_p)], axis=0))
            out = dot(a2p_ref[...], jnp.concatenate(parts, axis=1)).astype(BF16)
            for h in range(2):
                half = out[:, h * LANES:(h + 1) * LANES]
                u2send[t % RING, 2 * kp + h] = half[n_j:]
                u2keep[g % U2_RING, ab, 2 * kp + h] = half[:n_j]
            return carry

        lax.fori_loop(0, n_k // 2, body, 0, unroll=n_k // 2)

    def mode_one(n):
        g, part = place(n)

        def body(i, carry):
            k, j0 = i // (n_j // 16), i % (n_j // 16) * 16
            kk = part * k_part + k
            tiles = [u2keep[g % U2_RING, ab, kk, pl.ds(j0, 16)] for ab in range(n_ab)]
            tiles += [crecv[g % U2_RING * n_ab + ab, kk, pl.ds(j0, 16)] for ab in range(n_ab)]
            tiles = butterfly(tiles, 1)
            out = dot(jnp.concatenate(tiles, axis=0), a1p_ref[...]).astype(BF16).astype(F32)
            scale = d_ref[kk, pl.ds(j0, 16), :]
            out = (out.reshape(SG, 16, LANES) * scale[None]).astype(BF16)
            w_ref[pl.ds(g * SG, SG), kk, pl.ds(j0, 16), :] = out
            return carry

        lax.fori_loop(0, k_part * (n_j // 16), body, 0, unroll=8)

        @pl.when((part == n_ab - 1) & (g + U2_RING < n_g))
        def _():
            pl.semaphore_signal(free_sem, inc=1, device_id={"m1": 1 - m1}, device_id_type=MESH)

    def wait_core(g):
        each(n_ab, lambda ab: c_copy(index(g, ab)).wait_recv())

    first = PAIRED * n_ab + 1

    def step(t, carry):
        @pl.when((t + 3 >= PAIRED * n_ab) & (t + 3 < n_t))
        def _():
            each(n_p, lambda p: y_copy(t + 3, p).start())

        def piece(p, carry):
            @pl.when(t < n_t)
            def _():
                y_copy(t, p).wait_recv()

                @pl.when(t >= RING)
                def _():
                    x_copy(t - RING, p).wait_send()
                mode_three(t, p)
                x_copy(t, p).start()

                extra = ahead * (t + 1) + p

                @pl.when((p < ahead) & (extra < n_slab))
                def _():
                    regroup(extra)
            return carry

        lax.fori_loop(0, n_p, piece, 0)

        u = t - 1

        @pl.when(u >= 0)
        def _():
            each(n_p, lambda p: x_copy(u, p).wait_recv())

            @pl.when(u >= RING)
            def _():
                c_copy(u - RING).wait_send()
            mode_two(u)

            @pl.when((u % n_ab == 0) & (u >= U2_RING * n_ab))
            def _():
                pl.semaphore_wait(free_sem, 1)
            c_copy(u).start()

        z = t - first

        @pl.when((z >= 0) & (z < n_ab))
        def _():
            @pl.when(z == 0)
            def _():
                each(PAIRED, wait_core)
            each(PAIRED, lambda e: mode_one(z * PAIRED + e))

        @pl.when(z >= n_ab)
        def _():
            n = z - n_ab + PAIRED * n_ab

            @pl.when(z % n_ab == 0)
            def _():
                wait_core(n // n_ab)
            mode_one(n)
        return carry

    lax.fori_loop(0, n_t + 1, step, 0)

    wait_core(n_g - 1)
    each(n_ab, lambda i: mode_one(n_t - n_ab + i))

    def drain_y(t):
        each(n_p, lambda p: y_copy(t, p).wait_send())
    each(n_t, drain_y)

    def drain(i):
        t = n_t - RING + i
        each(n_p, lambda p: x_copy(t, p).wait_send())
        c_copy(t).wait_send()
    each(RING, drain)


def solution(mesh):
    def local_step(vol_blk, fac_one, fac_two, fac_three, diag_blk):
        n_s, n_a, n_b, n_l = vol_blk.shape
        n_k, n_j, n_i = diag_blk.shape
        x = jnp.transpose(vol_blk, (1, 2, 3, 0))
        n_g = n_s // SG // 2
        n_ab = n_a // AG
        n_t = n_g * n_ab
        n_p = n_b // PB
        vmem = pl.BlockSpec(memory_space=pltpu.VMEM)
        dma = pltpu.SemaphoreType.DMA
        return pl.pallas_call(
            kernel,
            out_shape=pltpu.VMEM((n_s // 2, n_k, n_j, n_i), BF16),
            in_specs=[pl.BlockSpec(memory_space=pl.ANY), vmem, vmem, vmem, vmem],
            out_specs=vmem,
            scratch_shapes=[
                pltpu.VMEM((RING, AG, PB, n_l, LANES), BF16),
                pltpu.VMEM((2 * n_g, n_ab, n_b, n_l, LANES), BF16),
                pltpu.VMEM((n_t, n_b, n_l, LANES), BF16),
                pltpu.VMEM((2, n_p, n_k, PB, LANES), BF16),
                pltpu.VMEM((RING, n_p, n_k, PB, LANES), BF16),
                pltpu.VMEM((n_t, n_p, n_k, PB, LANES), BF16),
                pltpu.VMEM((U2_RING, n_ab, n_k, n_j, LANES), BF16),
                pltpu.VMEM((RING, n_k, n_j, LANES), BF16),
                pltpu.VMEM((U2_RING * n_ab, n_k, n_j, LANES), BF16),
                pltpu.VMEM((fac_three.shape[0] * 8, 2 * 8 * n_l), BF16),
                pltpu.VMEM(fac_two.shape, BF16),
                pltpu.VMEM(fac_one.shape, BF16),
                dma((RING,)), pltpu.SemaphoreType.REGULAR,
                dma((n_t * n_p,)), dma((n_t * n_p,)),
                dma((RING * n_p,)), dma((n_t * n_p,)),
                dma((RING,)), dma((n_t,)),
            ],
            compiler_params=pltpu.CompilerParams(
                collective_id=0, has_side_effects=True, vmem_limit_bytes=47 * 1024 * 1024),
        )(x, fac_one, fac_two, fac_three, diag_blk)

    return jax.shard_map(local_step, mesh=mesh, in_specs=(P("dp", "m1", "m2", "m3"), P(), P(), P(), P("m2", "m1", None)), out_specs=P(("dp", "m3"), "m2", "m1", None), check_vma=False)
```

```python
import jax
import jax.numpy as jnp
from jax import lax
from jax.experimental import pallas as pl
from jax.experimental.pallas import tpu as pltpu
from jax.sharding import PartitionSpec as P

MESH = pl.DeviceIdType.MESH
F32, BF16 = jnp.float32, jnp.bfloat16

LANES = 128
SG = 8
AG = 16
PB = 16
SLAB_RING = 4
Y_RING = 6
X_RING = 4
C_RING = 4
G_RING = 3
Y_AHEAD = 2
PRE = 3
PER = 2


def skew(tiles, step):
    count = len(tiles)
    axis = tiles[0].ndim - 1
    block = lax.broadcasted_iota(jnp.int32, tiles[0].shape, axis) // step
    tiles = [t if i == 0 else pltpu.roll(t, i * step, axis) for i, t in enumerate(tiles)]
    dist = 1
    while dist < count:
        on = (block & dist) != 0
        tiles = [jnp.where(on, tiles[(h + dist) % count], tiles[h]) for h in range(count)]
        dist *= 2
    return [tiles[(count - g) % count] for g in range(count)]


def exchange(tiles, step):
    axis = tiles[0].ndim - 1
    return [t if g == 0 else pltpu.roll(t, LANES - g * step, axis) for g, t in enumerate(skew(tiles, step))]


def iota(shape, axis):
    return lax.broadcasted_iota(jnp.int32, shape, axis)


def one_hot(cond):
    return jnp.where(cond, 1.0, 0.0).astype(BF16)


def dot(a, b):
    return jnp.dot(a, b, preferred_element_type=F32)


def each(count, do):
    def body(i, carry):
        do(i)
        return carry
    lax.fori_loop(0, count, body, 0)


def kernel(x_hbm, a1_ref, a2_ref, a3_ref, d_ref, w_ref,
           slab, grp, yrecv, u3keep, u3send, xrecv, u2keep, u2send, crecv,
           l3_ref, a2p_ref, a1p_ref,
           slab_sem, free_sem, ysend_sem, yrecv_sem, xsend_sem, xrecv_sem, csend_sem, crecv_sem):
    m3, m2, m1 = lax.axis_index("m3"), lax.axis_index("m2"), lax.axis_index("m1")
    n_a, n_b, n_l, _ = x_hbm.shape
    n_ab = n_a // AG
    n_p = n_b // PB
    n_slab = n_ab * n_p
    n_g = grp.shape[0] // 2
    n_t = n_g * n_ab
    n_k = xrecv.shape[2]
    n_j = u2keep.shape[3]
    k_part = n_k // n_ab

    def slab_copy(i):
        return pltpu.make_async_copy(
            x_hbm.at[pl.ds(i // n_p * AG, AG), pl.ds(i % n_p * PB, PB)],
            slab.at[i % SLAB_RING], slab_sem.at[i % SLAB_RING])

    def y_copy(t, p):
        return pltpu.make_async_remote_copy(
            src_ref=grp.at[(1 - m3) * n_g + t // n_ab, t % n_ab, pl.ds(p * PB, PB)],
            dst_ref=yrecv.at[t, pl.ds(p * PB, PB)],
            send_sem=ysend_sem.at[t % Y_RING * n_p + p], recv_sem=yrecv_sem.at[t % Y_RING * n_p + p],
            device_id={"m3": 1 - m3}, device_id_type=MESH)

    def x_copy(t, p):
        return pltpu.make_async_remote_copy(
            src_ref=u3send.at[t % X_RING, p], dst_ref=xrecv.at[t, p],
            send_sem=xsend_sem.at[t % X_RING * n_p + p], recv_sem=xrecv_sem.at[t % X_RING * n_p + p],
            device_id={"m2": 1 - m2}, device_id_type=MESH)

    def c_copy(t):
        room = t % (G_RING * n_ab)
        return pltpu.make_async_remote_copy(
            src_ref=u2send.at[t % C_RING], dst_ref=crecv.at[room],
            send_sem=csend_sem.at[t % C_RING], recv_sem=crecv_sem.at[room],
            device_id={"m1": 1 - m1}, device_id_type=MESH)

    for i in range(SLAB_RING):
        slab_copy(i).start()

    barrier = pltpu.get_barrier_semaphore()
    for partner in ({"m3": 1 - m3}, {"m2": 1 - m2}, {"m1": 1 - m1}):
        pl.semaphore_signal(barrier, inc=1, device_id=partner, device_id_type=MESH)

    def regroup(i):
        ab, p = i // n_p, i % n_p
        slab_copy(i).wait()

        def one_b(b, carry):
            tiles = skew([slab[i % SLAB_RING, a, b] for a in range(AG)], SG)
            for g in range(2 * n_g):
                grp[g, ab, p * PB + b] = tiles[g]
            return carry

        lax.fori_loop(0, PB, one_b, 0, unroll=4)

        @pl.when(i + SLAB_RING < n_slab)
        def _():
            slab_copy(i + SLAB_RING).start()

    def regroup_send(i):
        regroup(i)
        y_copy(i // n_p, i % n_p).start()

    regroup(0)
    pl.semaphore_wait(barrier, 3)
    y_copy(0, 0).start()
    each(PRE - 1, lambda i: regroup_send(i + 1))

    k_all, l_all = a3_ref.shape
    rows = k_all * 8
    cols = 2 * 8 * n_l
    r, c = iota((rows, k_all), 0), iota((rows, k_all), 1)
    pick_k = one_hot((r // 8 + m2 * n_k) % k_all == c)
    r, c = iota((l_all, cols), 0), iota((l_all, cols), 1)
    pick_l = one_hot((c // (8 * n_l) + m3) % 2 * n_l + c % n_l == r)
    wide = dot(dot(pick_k, a3_ref[...]).astype(BF16), pick_l)
    r, c = iota((rows, cols), 0), iota((rows, cols), 1)
    l3_ref[...] = jnp.where(r % 8 == c // n_l % 8, wide, 0.0).astype(BF16)

    def order_two():
        size = a2_ref.shape[0]
        r, c = iota((size, size), 0), iota((size, size), 1)
        pick_j = one_hot((r + m1 * n_j) % size == c)
        pick_b = one_hot((c + m2 * n_b) % size == r)
        a2p_ref[...] = dot(dot(pick_j, a2_ref[...]).astype(BF16), pick_b).astype(BF16)

    def order_one(g):
        size = a1_ref.shape[0]
        r, c = iota((size, size), 0), iota((size, size), 1)
        v = r % (2 * n_ab)
        in_block = (r // (2 * n_ab) + 2 * n_g - (m3 * n_g + g)) % AG
        pick_a = one_hot((v // n_ab + m1) % 2 * n_a + v % n_ab * AG + in_block == c)
        a1p_ref[g] = lax.dot_general(pick_a, a1_ref[...], (((1,), (1,)), ((), ())),
                                     preferred_element_type=F32).astype(BF16)

    def mode_three(t, p):
        mine = m3 * n_g + t // n_ab
        parts = []
        for h in range(2):
            b0 = p * PB + 8 * h
            own = grp[mine, t % n_ab, pl.ds(b0, 8)].reshape(8 * n_l, LANES)
            got = yrecv[t, pl.ds(b0, 8)].reshape(8 * n_l, LANES)
            parts.append(jnp.concatenate([own, got], axis=0))
        out = dot(l3_ref[...], jnp.concatenate(parts, axis=1))
        lo = out[:, :LANES].reshape(2 * n_k, 8, LANES)
        hi = out[:, LANES:].reshape(2 * n_k, 8, LANES)
        full = jnp.concatenate([lo, hi], axis=1).astype(BF16)
        u3send[t % X_RING, p] = full[n_k:]
        u3keep[t % 2, p] = full[:n_k]

    def mode_two(t):
        g, ab = t // n_ab, t % n_ab

        def body(kp, carry):
            parts = []
            for k in (2 * kp, 2 * kp + 1):
                parts.append(jnp.concatenate([u3keep[t % 2, p, k] for p in range(n_p)]
                                             + [xrecv[t, p, k] for p in range(n_p)], axis=0))
            out = dot(a2p_ref[...], jnp.concatenate(parts, axis=1)).astype(BF16)
            for h in range(2):
                half = out[:, h * LANES:(h + 1) * LANES]
                u2send[t % C_RING, 2 * kp + h] = half[n_j:]
                u2keep[g % G_RING, ab, 2 * kp + h] = half[:n_j]
            return carry

        lax.fori_loop(0, n_k // 2, body, 0, unroll=n_k // 2)

    def mode_one(n):
        g, part = n // n_ab, n % n_ab
        slot = g % G_RING

        def body(i, carry):
            k, j0 = part * k_part + i // (n_j // 16), i % (n_j // 16) * 16
            tiles = [u2keep[slot, ab, k, pl.ds(j0, 16)] for ab in range(n_ab)]
            tiles += [crecv[slot * n_ab + ab, k, pl.ds(j0, 16)] for ab in range(n_ab)]
            tiles = exchange(tiles, 1)
            out = dot(jnp.concatenate(tiles, axis=0), a1p_ref[g]).astype(BF16).astype(F32)
            scale = d_ref[k, pl.ds(j0, 16), :]
            out = (out.reshape(SG, 16, LANES) * scale[None]).astype(BF16)
            w_ref[pl.ds(g * SG, SG), k, pl.ds(j0, 16), :] = out
            return carry

        count = k_part * (n_j // 16)
        lax.fori_loop(0, count, body, 0, unroll=count)

        @pl.when((part == n_ab - 1) & (g + G_RING < n_g))
        def _():
            pl.semaphore_signal(free_sem, inc=1, device_id={"m1": 1 - m1}, device_id_type=MESH)

    def wait_core(g):
        each(n_ab, lambda ab: c_copy(g * n_ab + ab).wait_recv())

    def step(t, carry):
        @pl.when((t + Y_AHEAD >= n_ab) & (t + Y_AHEAD < n_t))
        def _():
            @pl.when(t + Y_AHEAD >= Y_RING)
            def _():
                each(n_p, lambda p: y_copy(t + Y_AHEAD - Y_RING, p).wait_send())
            each(n_p, lambda p: y_copy(t + Y_AHEAD, p).start())

        def piece(p):
            y_copy(t, p).wait_recv()

            @pl.when(t >= X_RING)
            def _():
                x_copy(t - X_RING, p).wait_send()
            mode_three(t, p)
            x_copy(t, p).start()

            extra = PRE + PER * (t * n_p + p)

            @pl.when(extra < n_slab)
            def _():
                each(jnp.minimum(PER, n_slab - extra), lambda e: regroup_send(extra + e))

        @pl.when(t < n_t)
        def _():
            each(n_p, piece)

        @pl.when(t == 0)
        def _():
            order_two()

        u = t - 1

        @pl.when(u >= 0)
        def _():
            each(n_p, lambda p: x_copy(u, p).wait_recv())

            @pl.when(u >= C_RING)
            def _():
                c_copy(u - C_RING).wait_send()
            mode_two(u)

            @pl.when((u % n_ab == 0) & (u >= G_RING * n_ab))
            def _():
                pl.semaphore_wait(free_sem, 1)
            c_copy(u).start()

        @pl.when(t < n_g)
        def _():
            order_one(t)

        n = t - n_ab - 1

        @pl.when(n >= 0)
        def _():
            @pl.when(n % n_ab == 0)
            def _():
                wait_core(n // n_ab)
            mode_one(n)
        return carry

    lax.fori_loop(0, n_t + 1, step, 0)

    wait_core(n_g - 1)
    each(n_ab, lambda i: mode_one(n_t - n_ab + i))

    def drain_y(i):
        each(n_p, lambda p: y_copy(n_t - Y_RING + i, p).wait_send())
    each(Y_RING, drain_y)
    each(X_RING, lambda i: each(n_p, lambda p: x_copy(n_t - X_RING + i, p).wait_send()))
    each(C_RING, lambda i: c_copy(n_t - C_RING + i).wait_send())


def solution(mesh):
    def local_step(vol_blk, fac_one, fac_two, fac_three, diag_blk):
        n_s, n_a, n_b, n_l = vol_blk.shape
        n_k, n_j, n_i = diag_blk.shape
        x = jnp.transpose(vol_blk, (1, 2, 3, 0))
        n_g = n_s // SG // 2
        n_ab = n_a // AG
        n_t = n_g * n_ab
        n_p = n_b // PB
        vmem = pl.BlockSpec(memory_space=pltpu.VMEM)
        dma = pltpu.SemaphoreType.DMA
        return pl.pallas_call(
            kernel,
            out_shape=pltpu.VMEM((n_s // 2, n_k, n_j, n_i), BF16),
            in_specs=[pl.BlockSpec(memory_space=pl.ANY), vmem, vmem, vmem, vmem],
            out_specs=vmem,
            scratch_shapes=[
                pltpu.VMEM((SLAB_RING, AG, PB, n_l, LANES), BF16),
                pltpu.VMEM((2 * n_g, n_ab, n_b, n_l, LANES), BF16),
                pltpu.VMEM((n_t, n_b, n_l, LANES), BF16),
                pltpu.VMEM((2, n_p, n_k, PB, LANES), BF16),
                pltpu.VMEM((X_RING, n_p, n_k, PB, LANES), BF16),
                pltpu.VMEM((n_t, n_p, n_k, PB, LANES), BF16),
                pltpu.VMEM((G_RING, n_ab, n_k, n_j, LANES), BF16),
                pltpu.VMEM((C_RING, n_k, n_j, LANES), BF16),
                pltpu.VMEM((G_RING * n_ab, n_k, n_j, LANES), BF16),
                pltpu.VMEM((fac_three.shape[0] * 8, 2 * 8 * n_l), BF16),
                pltpu.VMEM(fac_two.shape, BF16),
                pltpu.VMEM((n_g,) + fac_one.shape, BF16),
                dma((SLAB_RING,)), pltpu.SemaphoreType.REGULAR,
                dma((Y_RING * n_p,)), dma((Y_RING * n_p,)),
                dma((X_RING * n_p,)), dma((X_RING * n_p,)),
                dma((C_RING,)), dma((G_RING * n_ab,)),
            ],
            compiler_params=pltpu.CompilerParams(
                collective_id=0, has_side_effects=True, vmem_limit_bytes=47 * 1024 * 1024),
        )(x, fac_one, fac_two, fac_three, diag_blk)

    return jax.shard_map(local_step, mesh=mesh, in_specs=(P("dp", "m1", "m2", "m3"), P(), P(), P(), P("m2", "m1", None)), out_specs=P(("dp", "m3"), "m2", "m1", None), check_vma=False)
```

```python
import jax
import jax.numpy as jnp
from jax import lax
from jax.experimental import pallas as pl
from jax.experimental.pallas import tpu as pltpu
from jax.sharding import PartitionSpec as P

MESH = pl.DeviceIdType.MESH
F32, BF16 = jnp.float32, jnp.bfloat16

LANES = 128
SG = 8
AG = 16
PB = 16
SLAB_RING = 4
Y_RING = 18
X_RING = 4
C_RING = 4
CR_RING = 12
Y_AHEAD = 8
PRE = 3
PER = 2


def skew(tiles, step):
    count = len(tiles)
    axis = tiles[0].ndim - 1
    block = lax.broadcasted_iota(jnp.int32, tiles[0].shape, axis) // step
    tiles = [t if i == 0 else pltpu.roll(t, i * step, axis) for i, t in enumerate(tiles)]
    dist = 1
    while dist < count:
        on = (block & dist) != 0
        tiles = [jnp.where(on, tiles[(h + dist) % count], tiles[h]) for h in range(count)]
        dist *= 2
    return [tiles[(count - g) % count] for g in range(count)]


def exchange(tiles, step):
    axis = tiles[0].ndim - 1
    return [t if g == 0 else pltpu.roll(t, LANES - g * step, axis) for g, t in enumerate(skew(tiles, step))]


def iota(shape, axis):
    return lax.broadcasted_iota(jnp.int32, shape, axis)


def one_hot(cond):
    return jnp.where(cond, 1.0, 0.0).astype(BF16)


def dot(a, b):
    return jnp.dot(a, b, preferred_element_type=F32)


def each(count, do):
    def body(i, carry):
        do(i)
        return carry
    lax.fori_loop(0, count, body, 0)


def mode_one_part(src, dst, a1p, d_ref, k_src, k_dst, count):
    n_jt = d_ref.shape[1] // 16

    def body(i, carry):
        k, rows = i // n_jt, pl.ds(i % n_jt * 16, 16)
        tiles = exchange([src[v, k_src + k, rows] for v in range(SG)], 1)
        out = dot(jnp.concatenate(tiles, axis=0), a1p).astype(BF16).astype(F32)
        out = out.reshape(SG, 16, LANES) * d_ref[k_src + k, rows, :][None]
        dst[:, k_dst + k, rows, :] = out.astype(BF16)
        return carry

    lax.fori_loop(0, count * n_jt, body, 0, unroll=count * n_jt)


def kernel(x_hbm, a1_ref, a2_ref, a3_ref, d_ref, w_ref, a1p_ref,
           slab, grp, yrecv, u3keep, u3send, xrecv, u2send,
           l3_ref, a2p_ref,
           slab_sem, ysend_sem, yrecv_sem, xsend_sem, xrecv_sem, csend_sem, crecv_sem):
    m3, m2, m1 = lax.axis_index("m3"), lax.axis_index("m2"), lax.axis_index("m1")
    n_a, n_b, n_l, _ = x_hbm.shape
    n_ab = n_a // AG
    n_p = n_b // PB
    n_slab = n_ab * n_p
    n_g = grp.shape[0] // 2
    n_t = n_g * n_ab
    n_k = xrecv.shape[2]
    n_j = u2send.shape[2]
    k_part = n_k // n_ab

    def slab_copy(i):
        return pltpu.make_async_copy(
            x_hbm.at[pl.ds(i // n_p * AG, AG), pl.ds(i % n_p * PB, PB)],
            slab.at[i % SLAB_RING], slab_sem.at[i % SLAB_RING])

    def y_copy(q):
        t, p = q // n_p, q % n_p
        return pltpu.make_async_remote_copy(
            src_ref=grp.at[(1 - m3) * n_g + t // n_ab, t % n_ab, pl.ds(p * PB, PB)],
            dst_ref=yrecv.at[t, pl.ds(p * PB, PB)],
            send_sem=ysend_sem.at[q % Y_RING], recv_sem=yrecv_sem.at[q % Y_RING],
            device_id={"m3": 1 - m3}, device_id_type=MESH)

    def x_copy(t, p):
        return pltpu.make_async_remote_copy(
            src_ref=u3send.at[t % X_RING, p], dst_ref=xrecv.at[t, p],
            send_sem=xsend_sem.at[t % X_RING * n_p + p], recv_sem=xrecv_sem.at[t % X_RING * n_p + p],
            device_id={"m2": 1 - m2}, device_id_type=MESH)

    def c_copy(t):
        return pltpu.make_async_remote_copy(
            src_ref=u2send.at[t % C_RING], dst_ref=w_ref.at[t // n_ab * SG + n_ab + t % n_ab],
            send_sem=csend_sem.at[t % C_RING], recv_sem=crecv_sem.at[t % CR_RING],
            device_id={"m1": 1 - m1}, device_id_type=MESH)

    slab_copy(0).start()

    barrier = pltpu.get_barrier_semaphore()
    for partner in ({"m3": 1 - m3}, {"m2": 1 - m2}, {"m1": 1 - m1}):
        pl.semaphore_signal(barrier, inc=1, device_id=partner, device_id_type=MESH)

    def regroup(i):
        ab, p = i // n_p, i % n_p
        def one_b(b, carry):
            tiles = skew([slab[i % SLAB_RING, a, b] for a in range(AG)], SG)
            for g in range(2 * n_g):
                grp[g, ab, p * PB + b] = tiles[g]
            return carry

        lax.fori_loop(0, PB, one_b, 0, unroll=4)

        @pl.when(i + SLAB_RING < n_slab)
        def _():
            slab_copy(i + SLAB_RING).start()

    def regroup_send(i):
        slab_copy(i).wait()
        regroup(i)
        y_copy(i).start()

    slab_copy(0).wait()
    for i in range(1, SLAB_RING):
        slab_copy(i).start()
    regroup(0)
    pl.semaphore_wait(barrier, 3)
    y_copy(0).start()
    each(PRE - 1, lambda i: regroup_send(i + 1))

    k_all, l_all = a3_ref.shape
    rows = k_all * 8
    cols = 2 * 8 * n_l
    r, c = iota((rows, k_all), 0), iota((rows, k_all), 1)
    pick_k = one_hot((r // 8 + m2 * n_k) % k_all == c)
    r, c = iota((l_all, cols), 0), iota((l_all, cols), 1)
    pick_l = one_hot((c // (8 * n_l) + m3) % 2 * n_l + c % n_l == r)
    wide = dot(dot(pick_k, a3_ref[...]).astype(BF16), pick_l)
    r, c = iota((rows, cols), 0), iota((rows, cols), 1)
    l3_ref[...] = jnp.where(r % 8 == c // n_l % 8, wide, 0.0).astype(BF16)

    def order_two():
        size = a2_ref.shape[0]
        r, c = iota((size, size), 0), iota((size, size), 1)
        pick_j = one_hot((r + m1 * n_j) % size == c)
        pick_b = one_hot((c + m2 * n_b) % size == r)
        a2p_ref[...] = dot(dot(pick_j, a2_ref[...]).astype(BF16), pick_b).astype(BF16)

    def order_one(g):
        size = a1_ref.shape[0]
        r, c = iota((size, size), 0), iota((size, size), 1)
        v = r % (2 * n_ab)
        in_block = (r // (2 * n_ab) + 2 * n_g - (m3 * n_g + g)) % AG
        pick_a = one_hot((v // n_ab + m1) % 2 * n_a + v % n_ab * AG + in_block == c)
        a1p_ref[g] = lax.dot_general(pick_a, a1_ref[...], (((1,), (1,)), ((), ())),
                                     preferred_element_type=F32).astype(BF16)

    def mode_three(t, p):
        mine = m3 * n_g + t // n_ab
        parts = []
        for h in range(2):
            b0 = p * PB + 8 * h
            own = grp[mine, t % n_ab, pl.ds(b0, 8)].reshape(8 * n_l, LANES)
            got = yrecv[t, pl.ds(b0, 8)].reshape(8 * n_l, LANES)
            parts.append(jnp.concatenate([own, got], axis=0))
        out = dot(l3_ref[...], jnp.concatenate(parts, axis=1))
        lo = out[:, :LANES].reshape(2 * n_k, 8, LANES)
        hi = out[:, LANES:].reshape(2 * n_k, 8, LANES)
        full = jnp.concatenate([lo, hi], axis=1).astype(BF16)
        u3send[t % X_RING, p] = full[n_k:]
        u3keep[t % 2, p] = full[:n_k]

    def mode_two(t):
        g, ab = t // n_ab, t % n_ab

        def body(kp, carry):
            parts = []
            for k in (2 * kp, 2 * kp + 1):
                parts.append(jnp.concatenate([u3keep[t % 2, p, k] for p in range(n_p)]
                                             + [xrecv[t, p, k] for p in range(n_p)], axis=0))
            out = dot(a2p_ref[...], jnp.concatenate(parts, axis=1)).astype(BF16)
            for h in range(2):
                half = out[:, h * LANES:(h + 1) * LANES]
                u2send[t % C_RING, 2 * kp + h] = half[n_j:]
                w_ref[g * SG + ab, 2 * kp + h] = half[:n_j]
            return carry

        lax.fori_loop(0, n_k // 2, body, 0, unroll=n_k // 2)

    def mode_one(n):
        g, part = n // n_ab, n % n_ab
        here = w_ref.at[pl.ds(g * SG, SG)]
        mode_one_part(here, here, a1p_ref[g], d_ref, part * k_part, part * k_part, k_part)

    def wait_core(g):
        each(n_ab, lambda ab: c_copy(g * n_ab + ab).wait_recv())

    def step(t, carry):
        def piece(p):
            q = t * n_p + p
            y_copy(q).wait_recv()

            @pl.when((q + Y_AHEAD >= n_slab) & (q + Y_AHEAD < n_t * n_p))
            def _():
                @pl.when(q + Y_AHEAD >= Y_RING)
                def _():
                    y_copy(q + Y_AHEAD - Y_RING).wait_send()
                y_copy(q + Y_AHEAD).start()

            @pl.when(t >= X_RING)
            def _():
                x_copy(t - X_RING, p).wait_send()
            mode_three(t, p)
            x_copy(t, p).start()

            extra = PRE + PER * q

            @pl.when(extra < n_slab)
            def _():
                each(jnp.minimum(PER, n_slab - extra), lambda e: regroup_send(extra + e))

        @pl.when(t < n_t)
        def _():
            each(n_p, piece)

        @pl.when(t == 0)
        def _():
            order_two()

        u = t - 1

        @pl.when(u >= 0)
        def _():
            each(n_p, lambda p: x_copy(u, p).wait_recv())

            @pl.when(u >= C_RING)
            def _():
                c_copy(u - C_RING).wait_send()
            mode_two(u)
            c_copy(u).start()

        @pl.when(t < n_g)
        def _():
            order_one(t)

        n = t - n_ab - 1

        @pl.when(n >= 0)
        def _():
            @pl.when(n % n_ab == 0)
            def _():
                wait_core(n // n_ab)
            mode_one(n)
        return carry

    lax.fori_loop(0, n_t + 1, step, 0)

    last = n_t * n_p - Y_RING
    each(Y_RING, lambda i: y_copy(last + i).wait_send())
    each(X_RING, lambda i: each(n_p, lambda p: x_copy(n_t - X_RING + i, p).wait_send()))
    each(C_RING, lambda i: c_copy(n_t - C_RING + i).wait_send())
    wait_core(n_g - 1)


def finish(w_vmem, a1p_ref, d_ref, w_hbm, wst, w_sem, last_sem):
    n_g = w_vmem.shape[0] // SG
    n_k = w_vmem.shape[1]
    parts = last_sem.shape[0]
    k_part = n_k // parts

    def group_copy(g):
        here = pl.ds(g * SG, SG)
        return pltpu.make_async_copy(w_vmem.at[here], w_hbm.at[here], w_sem.at[g])

    def part_copy(i):
        return pltpu.make_async_copy(
            wst.at[i], w_hbm.at[pl.ds((n_g - 1) * SG, SG), pl.ds(i * k_part, k_part)], last_sem.at[i])

    each(n_g - 1, lambda g: group_copy(g).start())
    a1p = a1p_ref[n_g - 1]

    def part(i):
        mode_one_part(w_vmem.at[pl.ds((n_g - 1) * SG, SG)], wst.at[i], a1p, d_ref, i * k_part, 0, k_part)
        part_copy(i).start()
    each(parts, part)
    each(n_g - 1, lambda g: group_copy(g).wait())
    each(parts, lambda i: part_copy(i).wait())


def solution(mesh):
    def local_step(vol_blk, fac_one, fac_two, fac_three, diag_blk):
        n_s, n_a, n_b, n_l = vol_blk.shape
        n_k, n_j, n_i = diag_blk.shape
        x = jnp.transpose(vol_blk, (1, 2, 3, 0))
        n_g = n_s // SG // 2
        n_ab = n_a // AG
        n_t = n_g * n_ab
        n_p = n_b // PB
        vmem = pl.BlockSpec(memory_space=pltpu.VMEM)
        dma = pltpu.SemaphoreType.DMA
        w_vmem, a1p = pl.pallas_call(
            kernel,
            out_shape=(pltpu.VMEM((n_s // 2, n_k, n_j, n_i), BF16), pltpu.VMEM((n_g,) + fac_one.shape, BF16)),
            in_specs=[pl.BlockSpec(memory_space=pl.ANY), vmem, vmem, vmem, vmem],
            out_specs=(vmem, vmem),
            scratch_shapes=[
                pltpu.VMEM((SLAB_RING, AG, PB, n_l, LANES), BF16),
                pltpu.VMEM((2 * n_g, n_ab, n_b, n_l, LANES), BF16),
                pltpu.VMEM((n_t, n_b, n_l, LANES), BF16),
                pltpu.VMEM((2, n_p, n_k, PB, LANES), BF16),
                pltpu.VMEM((X_RING, n_p, n_k, PB, LANES), BF16),
                pltpu.VMEM((n_t, n_p, n_k, PB, LANES), BF16),
                pltpu.VMEM((C_RING, n_k, n_j, LANES), BF16),
                pltpu.VMEM((fac_three.shape[0] * 8, 2 * 8 * n_l), BF16),
                pltpu.VMEM(fac_two.shape, BF16),
                dma((SLAB_RING,)),
                dma((Y_RING,)), dma((Y_RING,)),
                dma((X_RING * n_p,)), dma((X_RING * n_p,)),
                dma((C_RING,)), dma((CR_RING,)),
            ],
            compiler_params=pltpu.CompilerParams(
                collective_id=0, has_side_effects=True, vmem_limit_bytes=43 * 1024 * 1024),
        )(x, fac_one, fac_two, fac_three, diag_blk)
        return pl.pallas_call(
            finish,
            out_shape=jax.ShapeDtypeStruct(w_vmem.shape, BF16),
            in_specs=[vmem, vmem, vmem],
            out_specs=pl.BlockSpec(memory_space=pl.ANY),
            scratch_shapes=[pltpu.VMEM((n_ab, SG, n_k // n_ab, n_j, n_i), BF16), dma((n_g,)), dma((n_ab,))],
            compiler_params=pltpu.CompilerParams(vmem_limit_bytes=8 * 1024 * 1024),
        )(w_vmem, a1p, diag_blk)

    return jax.shard_map(local_step, mesh=mesh, in_specs=(P("dp", "m1", "m2", "m3"), P(), P(), P(), P("m2", "m1", None)), out_specs=P(("dp", "m3"), "m2", "m1", None), check_vma=False)
```

```python
import jax
import jax.numpy as jnp
from jax import lax
from jax.experimental import pallas as pl
from jax.experimental.pallas import tpu as pltpu
from jax.sharding import PartitionSpec as P

MESH = pl.DeviceIdType.MESH
F32, BF16 = jnp.float32, jnp.bfloat16

LANES = 128
SG = 8
AG = 16
PB = 8
SLAB_RING = 8
FIRST = 2
AHEAD = 8
Y_RING = 16
X_RING = 4
C_RING = 4
CG_RING = 3


def skew(tiles, step):
    count = len(tiles)
    axis = tiles[0].ndim - 1
    block = lax.broadcasted_iota(jnp.int32, tiles[0].shape, axis) // step
    tiles = [t if i == 0 else pltpu.roll(t, i * step, axis) for i, t in enumerate(tiles)]
    dist = 1
    while dist < count:
        on = (block & dist) != 0
        tiles = [jnp.where(on, tiles[(h + dist) % count], tiles[h]) for h in range(count)]
        dist *= 2
    return [tiles[(count - g) % count] for g in range(count)]


def exchange(tiles, step):
    axis = tiles[0].ndim - 1
    return [t if g == 0 else pltpu.roll(t, LANES - g * step, axis) for g, t in enumerate(skew(tiles, step))]


def iota(shape, axis):
    return lax.broadcasted_iota(jnp.int32, shape, axis)


def one_hot(cond):
    return jnp.where(cond, 1.0, 0.0).astype(BF16)


def dot(a, b):
    return jnp.dot(a, b, preferred_element_type=F32)


def each(count, do):
    def body(i, carry):
        do(i)
        return carry
    lax.fori_loop(0, count, body, 0)


def mode_one_part(src, dst, a1p, d_ref, k_src, k_dst, count):
    n_jt = d_ref.shape[1] // 16

    def body(i, carry):
        k, rows = i // n_jt, pl.ds(i % n_jt * 16, 16)
        tiles = exchange([src[v, k_src + k, rows] for v in range(SG)], 1)
        out = dot(jnp.concatenate(tiles, axis=0), a1p).astype(BF16).astype(F32)
        out = out.reshape(SG, 16, LANES) * d_ref[k_src + k, rows, :][None]
        dst[:, k_dst + k, rows, :] = out.astype(BF16)
        return carry

    lax.fori_loop(0, count * n_jt, body, 0, unroll=count * n_jt)


def kernel(x_hbm, a1_ref, a2_ref, a3_ref, d_ref, w_ref, a1p_ref,
           slab, grp, yrecv, u3keep, u3send, xrecv, u2send,
           l3_ref, a2p_ref,
           slab_sem, ysend_sem, yrecv_sem, xsend_sem, xrecv_sem, csend_sem, crecv_sem):
    m3, m2, m1 = lax.axis_index("m3"), lax.axis_index("m2"), lax.axis_index("m1")
    n_a, n_b, n_l, _ = x_hbm.shape
    n_ab = n_a // AG
    n_p = n_b // PB
    n_slab = n_ab * n_p
    n_g = grp.shape[0] // 2
    n_t = n_g * n_ab
    n_k = xrecv.shape[2]
    n_j = u2send.shape[2]
    k_part = n_k // n_ab

    def slab_copy(i):
        return pltpu.make_async_copy(
            x_hbm.at[pl.ds(i // n_p * AG, AG), pl.ds(i % n_p * PB, PB)],
            slab.at[i % SLAB_RING], slab_sem.at[i % SLAB_RING])

    def remote(axis, src, dst, send_sem, recv_sem):
        return pltpu.make_async_remote_copy(
            src_ref=src, dst_ref=dst, send_sem=send_sem, recv_sem=recv_sem,
            device_id={axis: 1 - lax.axis_index(axis)}, device_id_type=MESH)

    def y_copy(q):
        t, p = q // n_p, q % n_p
        return remote("m3", grp.at[(1 - m3) * n_g + t // n_ab, t % n_ab, pl.ds(p * PB, PB)],
                      yrecv.at[t // n_ab, t % n_ab, pl.ds(p * PB, PB)], ysend_sem, yrecv_sem.at[q % Y_RING])

    def y_all():
        return remote("m3", grp.at[pl.ds((1 - m3) * n_g, n_g)], yrecv, ysend_sem, yrecv_sem.at[0])

    def x_copy(t, p):
        return remote("m2", u3send.at[t % X_RING, p], xrecv.at[t, p],
                      xsend_sem.at[t % X_RING], xrecv_sem.at[t % X_RING])

    def x_all(t):
        return remote("m2", u3send.at[t % X_RING], xrecv.at[t],
                      xsend_sem.at[t % X_RING], xrecv_sem.at[t % X_RING])

    def c_copy(t, ks):
        g = t // n_ab
        return remote("m1", u2send.at[t % C_RING, ks], w_ref.at[g * SG + n_ab + t % n_ab, ks],
                      csend_sem.at[t % C_RING], crecv_sem.at[g % CG_RING])

    def c_sent(t):
        return c_copy(t, pl.ds(0, n_k))

    def c_group(g):
        here = w_ref.at[pl.ds(g * SG + n_ab, n_ab)]
        return remote("m1", here, here, csend_sem.at[0], crecv_sem.at[g % CG_RING])

    for i in range(FIRST):
        slab_copy(i).start()

    barrier = pltpu.get_barrier_semaphore()
    for partner in ({"m3": 1 - m3}, {"m2": 1 - m2}, {"m1": 1 - m1}):
        pl.semaphore_signal(barrier, inc=1, device_id=partner, device_id_type=MESH)

    def regroup(i):
        ab, p = i // n_p, i % n_p
        def one_b(b, carry):
            tiles = skew([slab[i % SLAB_RING, a, b] for a in range(AG)], SG)
            for g in range(2 * n_g):
                grp[g, ab, p * PB + b] = tiles[g]
            return carry

        lax.fori_loop(0, PB, one_b, 0, unroll=4)

        @pl.when(i + SLAB_RING < n_slab)
        def _():
            slab_copy(i + SLAB_RING).start()

    slab_copy(0).wait()
    for i in range(FIRST, SLAB_RING):
        slab_copy(i).start()
    regroup(0)
    pl.semaphore_wait(barrier, 3)
    y_copy(0).start()

    def next_piece(i):
        @pl.when(i < n_slab)
        def _():
            slab_copy(i).wait()
            regroup(i)
        y_copy(i).start()

    each(AHEAD - 1, lambda i: next_piece(i + 1))

    k_all, l_all = a3_ref.shape
    rows = k_all * 8
    cols = 2 * 8 * n_l
    r, c = iota((rows, k_all), 0), iota((rows, k_all), 1)
    pick_k = one_hot((r // 8 + m2 * n_k) % k_all == c)
    r, c = iota((l_all, cols), 0), iota((l_all, cols), 1)
    pick_l = one_hot((c // (8 * n_l) + m3) % 2 * n_l + c % n_l == r)
    wide = dot(dot(pick_k, a3_ref[...]).astype(BF16), pick_l)
    r, c = iota((rows, cols), 0), iota((rows, cols), 1)
    l3_ref[...] = jnp.where(r % 8 == c // n_l % 8, wide, 0.0).astype(BF16)

    def order_two():
        size = a2_ref.shape[0]
        r, c = iota((size, size), 0), iota((size, size), 1)
        pick_j = one_hot((r + m1 * n_j) % size == c)
        pick_b = one_hot((c + m2 * n_b) % size == r)
        a2p_ref[...] = dot(dot(pick_j, a2_ref[...]).astype(BF16), pick_b).astype(BF16)

    def order_one(g):
        size = a1_ref.shape[0]
        r, c = iota((size, size), 0), iota((size, size), 1)
        v = r % (2 * n_ab)
        in_block = (r // (2 * n_ab) + 2 * n_g - (m3 * n_g + g)) % AG
        pick_a = one_hot((v // n_ab + m1) % 2 * n_a + v % n_ab * AG + in_block == c)
        a1p_ref[g] = lax.dot_general(pick_a, a1_ref[...], (((1,), (1,)), ((), ())),
                                     preferred_element_type=F32).astype(BF16)

    def mode_three(t, p):
        g, ab, rows = t // n_ab, t % n_ab, pl.ds(p * PB, PB)
        own = grp[m3 * n_g + g, ab, rows].reshape(PB * n_l, LANES)
        got = yrecv[g, ab, rows].reshape(PB * n_l, LANES)
        out = dot(l3_ref[...], jnp.concatenate([own, got], axis=0))
        out = out.reshape(2 * n_k, PB, LANES).astype(BF16)
        u3send[t % X_RING, p] = out[n_k:]
        u3keep[t % 2, p] = out[:n_k]

    def mode_two(t):
        g, ab = t // n_ab, t % n_ab
        for part in range(n_ab):
            for kp in range(part * k_part, (part + 1) * k_part, 2):
                cols = []
                for k in (kp, kp + 1):
                    cols.append(jnp.concatenate([u3keep[t % 2, :, k].reshape(n_b, LANES),
                                                 xrecv[t, :, k].reshape(n_b, LANES)], axis=0))
                out = dot(a2p_ref[...], jnp.concatenate(cols, axis=1)).astype(BF16)
                for h in range(2):
                    half = out[:, h * LANES:(h + 1) * LANES]
                    u2send[t % C_RING, kp + h] = half[n_j:]
                    w_ref[g * SG + ab, kp + h] = half[:n_j]
            c_copy(t, pl.ds(part * k_part, k_part)).start()

    def mode_one(n):
        g, part = n // n_ab, n % n_ab
        here = w_ref.at[pl.ds(g * SG, SG)]
        mode_one_part(here, here, a1p_ref[g], d_ref, part * k_part, part * k_part, k_part)

    def step(t, carry):
        @pl.when((t >= X_RING) & (t < n_t))
        def _():
            x_all(t - X_RING).wait_send()

        def piece(p):
            q = t * n_p + p
            y_copy(q).wait_recv()
            mode_three(t, p)
            x_copy(t, p).start()

            @pl.when(q + AHEAD < n_t * n_p)
            def _():
                next_piece(q + AHEAD)

        @pl.when(t < n_t)
        def _():
            each(n_p, piece)

        @pl.when(t == 0)
        def _():
            order_two()

        u = t - 1

        @pl.when(u >= 0)
        def _():
            x_all(u).wait_recv()

            @pl.when(u >= C_RING)
            def _():
                c_sent(u - C_RING).wait_send()
            mode_two(u)

        @pl.when(t < n_g)
        def _():
            order_one(t)

        n = t - n_ab - 1

        @pl.when(n >= 0)
        def _():
            @pl.when(n % n_ab == 0)
            def _():
                c_group(n // n_ab).wait_recv()
            mode_one(n)
        return carry

    lax.fori_loop(0, n_t + 1, step, 0)

    y_all().wait_send()
    each(X_RING, lambda i: x_all(n_t - X_RING + i).wait_send())
    each(C_RING, lambda i: c_sent(n_t - C_RING + i).wait_send())
    c_group(n_g - 1).wait_recv()


def finish(w_vmem, a1p_ref, d_ref, w_hbm, wst, w_sem, last_sem):
    n_g = w_vmem.shape[0] // SG
    n_k = w_vmem.shape[1]
    parts = last_sem.shape[0]
    k_part = n_k // parts

    def group_copy(g):
        here = pl.ds(g * SG, SG)
        return pltpu.make_async_copy(w_vmem.at[here], w_hbm.at[here], w_sem.at[g])

    def part_copy(i):
        return pltpu.make_async_copy(
            wst.at[i], w_hbm.at[pl.ds((n_g - 1) * SG, SG), pl.ds(i * k_part, k_part)], last_sem.at[i])

    each(n_g - 1, lambda g: group_copy(g).start())
    a1p = a1p_ref[n_g - 1]

    def part(i):
        mode_one_part(w_vmem.at[pl.ds((n_g - 1) * SG, SG)], wst.at[i], a1p, d_ref, i * k_part, 0, k_part)
        part_copy(i).start()
    each(parts, part)
    each(n_g - 1, lambda g: group_copy(g).wait())
    each(parts, lambda i: part_copy(i).wait())


def solution(mesh):
    def local_step(vol_blk, fac_one, fac_two, fac_three, diag_blk):
        n_s, n_a, n_b, n_l = vol_blk.shape
        n_k, n_j, n_i = diag_blk.shape
        x = jnp.transpose(vol_blk, (1, 2, 3, 0))
        n_g = n_s // SG // 2
        n_ab = n_a // AG
        n_t = n_g * n_ab
        n_p = n_b // PB
        vmem = pl.BlockSpec(memory_space=pltpu.VMEM)
        dma = pltpu.SemaphoreType.DMA
        w_vmem, a1p = pl.pallas_call(
            kernel,
            out_shape=(pltpu.VMEM((n_s // 2, n_k, n_j, n_i), BF16), pltpu.VMEM((n_g,) + fac_one.shape, BF16)),
            in_specs=[pl.BlockSpec(memory_space=pl.ANY), vmem, vmem, vmem, vmem],
            out_specs=(vmem, vmem),
            scratch_shapes=[
                pltpu.VMEM((SLAB_RING, AG, PB, n_l, LANES), BF16),
                pltpu.VMEM((2 * n_g, n_ab, n_b, n_l, LANES), BF16),
                pltpu.VMEM((n_g, n_ab, n_b, n_l, LANES), BF16),
                pltpu.VMEM((2, n_p, n_k, PB, LANES), BF16),
                pltpu.VMEM((X_RING, n_p, n_k, PB, LANES), BF16),
                pltpu.VMEM((n_t, n_p, n_k, PB, LANES), BF16),
                pltpu.VMEM((C_RING, n_k, n_j, LANES), BF16),
                pltpu.VMEM((fac_three.shape[0] * 8, 2 * 8 * n_l), BF16),
                pltpu.VMEM(fac_two.shape, BF16),
                dma((SLAB_RING,)),
                dma, dma((Y_RING,)),
                dma((X_RING,)), dma((X_RING,)),
                dma((C_RING,)), dma((CG_RING,)),
            ],
            compiler_params=pltpu.CompilerParams(
                collective_id=0, has_side_effects=True, vmem_limit_bytes=43 * 1024 * 1024),
        )(x, fac_one, fac_two, fac_three, diag_blk)
        return pl.pallas_call(
            finish,
            out_shape=jax.ShapeDtypeStruct(w_vmem.shape, BF16),
            in_specs=[vmem, vmem, vmem],
            out_specs=pl.BlockSpec(memory_space=pl.ANY),
            scratch_shapes=[pltpu.VMEM((n_ab, SG, n_k // n_ab, n_j, n_i), BF16), dma((n_g,)), dma((n_ab,))],
            compiler_params=pltpu.CompilerParams(vmem_limit_bytes=8 * 1024 * 1024),
        )(w_vmem, a1p, diag_blk)

    return jax.shard_map(local_step, mesh=mesh, in_specs=(P("dp", "m1", "m2", "m3"), P(), P(), P(), P("m2", "m1", None)), out_specs=P(("dp", "m3"), "m2", "m1", None), check_vma=False)
```

```python
import jax
import jax.numpy as jnp
from jax import lax
from jax.experimental import pallas as pl
from jax.experimental.pallas import tpu as pltpu
from jax.sharding import PartitionSpec as P

MESH = pl.DeviceIdType.MESH
F32, BF16 = jnp.float32, jnp.bfloat16

LANES = 128
SG = 8
AG = 16
PB = 8
SLAB_RING = 4
FIRST = 4
AHEAD = 7
Y_RING = 14
X_RING = 4
C_RING = 2
CG_RING = 3


def skew(tiles, step):
    count = len(tiles)
    axis = tiles[0].ndim - 1
    block = lax.broadcasted_iota(jnp.int32, tiles[0].shape, axis) // step
    tiles = [t if i == 0 else pltpu.roll(t, i * step, axis) for i, t in enumerate(tiles)]
    dist = 1
    while dist < count:
        on = (block & dist) != 0
        tiles = [jnp.where(on, tiles[(h + dist) % count], tiles[h]) for h in range(count)]
        dist *= 2
    return [tiles[(count - g) % count] for g in range(count)]


def exchange(tiles, step):
    axis = tiles[0].ndim - 1
    return [t if g == 0 else pltpu.roll(t, LANES - g * step, axis) for g, t in enumerate(skew(tiles, step))]


def iota(shape, axis):
    return lax.broadcasted_iota(jnp.int32, shape, axis)


def one_hot(cond):
    return jnp.where(cond, 1.0, 0.0).astype(BF16)


def dot(a, b):
    return jnp.dot(a, b, preferred_element_type=F32)


def each(count, do):
    def body(i, carry):
        do(i)
        return carry
    lax.fori_loop(0, count, body, 0)


def mode_one_part(src, dst, a1p, d_ref, k_src, k_dst, count):
    n_jt = d_ref.shape[1] // 16

    def body(i, carry):
        k, rows = i // n_jt, pl.ds(i % n_jt * 16, 16)
        tiles = exchange([src[v, k_src + k, rows] for v in range(SG)], 1)
        out = dot(jnp.concatenate(tiles, axis=0), a1p).astype(BF16).astype(F32)
        out = out.reshape(SG, 16, LANES) * d_ref[k_src + k, rows, :][None]
        dst[:, k_dst + k, rows, :] = out.astype(BF16)
        return carry

    lax.fori_loop(0, count * n_jt, body, 0, unroll=count * n_jt)


def kernel(x_hbm, a1_ref, a2_ref, a3_ref, d_ref, w_ref, a1p_ref,
           slab, grp, yrecv, u3keep, u3send, xrecv, u2send,
           l3_ref, a2p_ref,
           slab_sem, ysend_sem, yrecv_sem, xsend_sem, xrecv_sem, csend_sem, crecv_sem):
    m3, m2, m1 = lax.axis_index("m3"), lax.axis_index("m2"), lax.axis_index("m1")
    n_a, n_b, n_l, _ = x_hbm.shape
    n_ab = n_a // AG
    n_p = n_b // PB
    n_slab = n_ab * n_p
    n_g = grp.shape[0] // 2
    n_t = n_g * n_ab
    n_k = xrecv.shape[2]
    n_j = u2send.shape[2]
    k_part = n_k // n_ab

    def slab_copy(i):
        return pltpu.make_async_copy(
            x_hbm.at[pl.ds(i // n_p * AG, AG), pl.ds(i % n_p * PB, PB)],
            slab.at[i % SLAB_RING], slab_sem.at[i % SLAB_RING])

    def remote(axis, src, dst, send_sem, recv_sem):
        return pltpu.make_async_remote_copy(
            src_ref=src, dst_ref=dst, send_sem=send_sem, recv_sem=recv_sem,
            device_id={axis: 1 - lax.axis_index(axis)}, device_id_type=MESH)

    def y_copy(q):
        t, p = q // n_p, q % n_p
        return remote("m3", grp.at[(1 - m3) * n_g + t // n_ab, t % n_ab, pl.ds(p * PB, PB)],
                      yrecv.at[t // n_ab, t % n_ab, pl.ds(p * PB, PB)], ysend_sem, yrecv_sem.at[q % Y_RING])

    def y_all():
        return remote("m3", grp.at[pl.ds((1 - m3) * n_g, n_g)], yrecv, ysend_sem, yrecv_sem.at[0])

    def x_copy(t, p):
        return remote("m2", u3send.at[t % X_RING, p], xrecv.at[t, p],
                      xsend_sem.at[t % X_RING], xrecv_sem.at[t % X_RING])

    def x_all(t):
        return remote("m2", u3send.at[t % X_RING], xrecv.at[t],
                      xsend_sem.at[t % X_RING], xrecv_sem.at[t % X_RING])

    def c_copy(t):
        g = t // n_ab
        return remote("m1", u2send.at[t % C_RING], w_ref.at[g * SG + n_ab + t % n_ab],
                      csend_sem.at[t % C_RING], crecv_sem.at[g % CG_RING])

    def c_group(g):
        here = w_ref.at[pl.ds(g * SG + n_ab, n_ab)]
        return remote("m1", here, here, csend_sem.at[0], crecv_sem.at[g % CG_RING])

    for i in range(FIRST):
        slab_copy(i).start()

    barrier = pltpu.get_barrier_semaphore()
    for partner in ({"m3": 1 - m3}, {"m2": 1 - m2}, {"m1": 1 - m1}):
        pl.semaphore_signal(barrier, inc=1, device_id=partner, device_id_type=MESH)

    def regroup(i):
        ab, p = i // n_p, i % n_p
        def one_b(b, carry):
            tiles = skew([slab[i % SLAB_RING, a, b] for a in range(AG)], SG)
            for g in range(2 * n_g):
                grp[g, ab, p * PB + b] = tiles[g]
            return carry

        lax.fori_loop(0, PB, one_b, 0, unroll=8)

        @pl.when(i + SLAB_RING < n_slab)
        def _():
            slab_copy(i + SLAB_RING).start()

    slab_copy(0).wait()
    for i in range(FIRST, SLAB_RING):
        slab_copy(i).start()
    regroup(0)
    pl.semaphore_wait(barrier, 3)
    y_copy(0).start()

    def next_piece(i):
        @pl.when(i < n_slab)
        def _():
            slab_copy(i).wait()
            regroup(i)
        y_copy(i).start()

    each(AHEAD - 1, lambda i: next_piece(i + 1))

    k_all, l_all = a3_ref.shape
    rows = k_all * 8
    cols = 2 * 8 * n_l
    r, c = iota((rows, k_all), 0), iota((rows, k_all), 1)
    pick_k = one_hot((r // 8 + m2 * n_k) % k_all == c)
    r, c = iota((l_all, cols), 0), iota((l_all, cols), 1)
    pick_l = one_hot((c // (8 * n_l) + m3) % 2 * n_l + c % n_l == r)
    wide = dot(dot(pick_k, a3_ref[...]).astype(BF16), pick_l)
    r, c = iota((rows, cols), 0), iota((rows, cols), 1)
    l3_ref[...] = jnp.where(r % 8 == c // n_l % 8, wide, 0.0).astype(BF16)

    def order_two():
        size = a2_ref.shape[0]
        r, c = iota((size, size), 0), iota((size, size), 1)
        pick_j = one_hot((r + m1 * n_j) % size == c)
        pick_b = one_hot((c + m2 * n_b) % size == r)
        a2p_ref[...] = dot(dot(pick_j, a2_ref[...]).astype(BF16), pick_b).astype(BF16)

    def order_one(g):
        size = a1_ref.shape[0]
        r, c = iota((size, size), 0), iota((size, size), 1)
        v = r % (2 * n_ab)
        in_block = (r // (2 * n_ab) + 2 * n_g - (m3 * n_g + g)) % AG
        pick_a = one_hot((v // n_ab + m1) % 2 * n_a + v % n_ab * AG + in_block == c)
        a1p_ref[g] = lax.dot_general(pick_a, a1_ref[...], (((1,), (1,)), ((), ())),
                                     preferred_element_type=F32).astype(BF16)

    def mode_three(t, p):
        g, ab, rows = t // n_ab, t % n_ab, pl.ds(p * PB, PB)
        own = grp[m3 * n_g + g, ab, rows].reshape(PB * n_l, LANES)
        got = yrecv[g, ab, rows].reshape(PB * n_l, LANES)
        out = dot(l3_ref[...], jnp.concatenate([own, got], axis=0))
        out = out.reshape(2 * n_k, PB, LANES).astype(BF16)
        u3send[t % X_RING, p] = out[n_k:]
        u3keep[t % 2, p] = out[:n_k]

    def mode_two(t):
        g, ab = t // n_ab, t % n_ab
        for kp in range(0, n_k, 2):
            cols = []
            for k in (kp, kp + 1):
                cols.append(jnp.concatenate([u3keep[t % 2, :, k].reshape(n_b, LANES),
                                             xrecv[t, :, k].reshape(n_b, LANES)], axis=0))
            out = dot(a2p_ref[...], jnp.concatenate(cols, axis=1)).astype(BF16)
            for h in range(2):
                half = out[:, h * LANES:(h + 1) * LANES]
                u2send[t % C_RING, kp + h] = half[n_j:]
                w_ref[g * SG + ab, kp + h] = half[:n_j]
        c_copy(t).start()

    def mode_one(n):
        g, part = n // n_ab, n % n_ab
        here = w_ref.at[pl.ds(g * SG, SG)]
        mode_one_part(here, here, a1p_ref[g], d_ref, part * k_part, part * k_part, k_part)

    def step(t, carry):
        @pl.when((t >= X_RING) & (t < n_t))
        def _():
            x_all(t - X_RING).wait_send()

        def piece(p):
            q = t * n_p + p
            y_copy(q).wait_recv()
            mode_three(t, p)
            x_copy(t, p).start()

            @pl.when(q + AHEAD < n_t * n_p)
            def _():
                next_piece(q + AHEAD)

        @pl.when(t < n_t)
        def _():
            each(n_p, piece)

        @pl.when(t == 0)
        def _():
            order_two()

        u = t - 1

        @pl.when(u >= 0)
        def _():
            x_all(u).wait_recv()

            @pl.when(u >= C_RING)
            def _():
                c_copy(u - C_RING).wait_send()
            mode_two(u)

        @pl.when(t < n_g)
        def _():
            order_one(t)

        n = t - n_ab - 1

        @pl.when(n >= 0)
        def _():
            @pl.when(n % n_ab == 0)
            def _():
                c_group(n // n_ab).wait_recv()
            mode_one(n)
        return carry

    lax.fori_loop(0, n_t + 1, step, 0)

    y_all().wait_send()
    each(X_RING, lambda i: x_all(n_t - X_RING + i).wait_send())
    each(C_RING, lambda i: c_copy(n_t - C_RING + i).wait_send())
    c_group(n_g - 1).wait_recv()


def finish(w_vmem, a1p_ref, d_ref, w_hbm, wst, w_sem, last_sem):
    n_g = w_vmem.shape[0] // SG
    n_k = w_vmem.shape[1]
    parts = wst.shape[0]
    k_part = n_k // parts

    def group_copy(g):
        here = pl.ds(g * SG, SG)
        return pltpu.make_async_copy(w_vmem.at[here], w_hbm.at[here], w_sem)

    def part_copy(i):
        return pltpu.make_async_copy(
            wst.at[i], w_hbm.at[pl.ds((n_g - 1) * SG, SG), pl.ds(i * k_part, k_part)], last_sem)

    each(n_g - 1, lambda g: group_copy(g).start())
    a1p = a1p_ref[n_g - 1]

    def part(i):
        mode_one_part(w_vmem.at[pl.ds((n_g - 1) * SG, SG)], wst.at[i], a1p, d_ref, i * k_part, 0, k_part)
        part_copy(i).start()
    each(parts, part)
    most = pl.ds(0, (n_g - 1) * SG)
    pltpu.make_async_copy(w_vmem.at[most], w_hbm.at[most], w_sem).wait()
    last = pl.ds((n_g - 1) * SG, SG)
    pltpu.make_async_copy(w_vmem.at[last], w_hbm.at[last], last_sem).wait()


def solution(mesh):
    def local_step(vol_blk, fac_one, fac_two, fac_three, diag_blk):
        n_s, n_a, n_b, n_l = vol_blk.shape
        n_k, n_j, n_i = diag_blk.shape
        x = jnp.transpose(vol_blk, (1, 2, 3, 0))
        n_g = n_s // SG // 2
        n_ab = n_a // AG
        n_t = n_g * n_ab
        n_p = n_b // PB
        vmem = pl.BlockSpec(memory_space=pltpu.VMEM)
        dma = pltpu.SemaphoreType.DMA
        w_vmem, a1p = pl.pallas_call(
            kernel,
            out_shape=(pltpu.VMEM((n_s // 2, n_k, n_j, n_i), BF16), pltpu.VMEM((n_g,) + fac_one.shape, BF16)),
            in_specs=[pl.BlockSpec(memory_space=pl.ANY), vmem, vmem, vmem, vmem],
            out_specs=(vmem, vmem),
            scratch_shapes=[
                pltpu.VMEM((SLAB_RING, AG, PB, n_l, LANES), BF16),
                pltpu.VMEM((2 * n_g, n_ab, n_b, n_l, LANES), BF16),
                pltpu.VMEM((n_g, n_ab, n_b, n_l, LANES), BF16),
                pltpu.VMEM((2, n_p, n_k, PB, LANES), BF16),
                pltpu.VMEM((X_RING, n_p, n_k, PB, LANES), BF16),
                pltpu.VMEM((n_t, n_p, n_k, PB, LANES), BF16),
                pltpu.VMEM((C_RING, n_k, n_j, LANES), BF16),
                pltpu.VMEM((fac_three.shape[0] * 8, 2 * 8 * n_l), BF16),
                pltpu.VMEM(fac_two.shape, BF16),
                dma((SLAB_RING,)),
                dma, dma((Y_RING,)),
                dma((X_RING,)), dma((X_RING,)),
                dma((C_RING,)), dma((CG_RING,)),
            ],
            compiler_params=pltpu.CompilerParams(
                collective_id=0, has_side_effects=True, vmem_limit_bytes=43 * 1024 * 1024),
        )(x, fac_one, fac_two, fac_three, diag_blk)
        return pl.pallas_call(
            finish,
            out_shape=jax.ShapeDtypeStruct(w_vmem.shape, BF16),
            in_specs=[vmem, vmem, vmem],
            out_specs=pl.BlockSpec(memory_space=pl.ANY),
            scratch_shapes=[pltpu.VMEM((n_ab, SG, n_k // n_ab, n_j, n_i), BF16), dma, dma],
            compiler_params=pltpu.CompilerParams(vmem_limit_bytes=8 * 1024 * 1024),
        )(w_vmem, a1p, diag_blk)

    return jax.shard_map(local_step, mesh=mesh, in_specs=(P("dp", "m1", "m2", "m3"), P(), P(), P(), P("m2", "m1", None)), out_specs=P(("dp", "m3"), "m2", "m1", None), check_vma=False)
```

```python
import jax
import jax.numpy as jnp
from jax import lax
from jax.experimental import pallas as pl
from jax.experimental.pallas import tpu as pltpu
from jax.sharding import PartitionSpec as P

MESH = pl.DeviceIdType.MESH
F32, BF16 = jnp.float32, jnp.bfloat16

LANES = 128
SG = 8
AG = 16
PB = 8
SLAB_RING = 4
FIRST = 4
AHEAD = 7
Y_RING = 14
X_RING = 4
C_RING = 2
CG_RING = 3


def skew(tiles, step):
    count = len(tiles)
    axis = tiles[0].ndim - 1
    block = lax.broadcasted_iota(jnp.int32, tiles[0].shape, axis) // step
    tiles = [t if i == 0 else pltpu.roll(t, i * step, axis) for i, t in enumerate(tiles)]
    dist = 1
    while dist < count:
        on = (block & dist) != 0
        tiles = [jnp.where(on, tiles[(h + dist) % count], tiles[h]) for h in range(count)]
        dist *= 2
    return [tiles[(count - g) % count] for g in range(count)]


def exchange(tiles, step):
    axis = tiles[0].ndim - 1
    return [t if g == 0 else pltpu.roll(t, LANES - g * step, axis) for g, t in enumerate(skew(tiles, step))]


def iota(shape, axis):
    return lax.broadcasted_iota(jnp.int32, shape, axis)


def one_hot(cond):
    return jnp.where(cond, 1.0, 0.0).astype(BF16)


def dot(a, b):
    return jnp.dot(a, b, preferred_element_type=F32)


def each(count, do):
    def body(i, carry):
        do(i)
        return carry
    lax.fori_loop(0, count, body, 0)


def mode_one_part(src, dst, a1p, d_ref, k_src, k_dst, count):
    n_jt = d_ref.shape[1] // 16

    def body(i, carry):
        k, rows = i // n_jt, pl.ds(i % n_jt * 16, 16)
        tiles = exchange([src[v, k_src + k, rows] for v in range(SG)], 1)
        out = dot(jnp.concatenate(tiles, axis=0), a1p).astype(BF16).astype(F32)
        out = out.reshape(SG, 16, LANES) * d_ref[k_src + k, rows, :][None]
        dst[:, k_dst + k, rows, :] = out.astype(BF16)
        return carry

    lax.fori_loop(0, count * n_jt, body, 0, unroll=count * n_jt)


def kernel(x_hbm, a1_hbm, a2_hbm, a3_hbm, d_hbm, w_ref, a1p_ref, d_ref,
           slab, grp, yrecv, u3keep, u3send, xrecv, u2send,
           a1_ref, a2_ref, a3_ref, l3_ref, a2p_ref,
           fac_sem, slab_sem, ysend_sem, yrecv_sem, xsend_sem, xrecv_sem, csend_sem, crecv_sem):
    m3, m2, m1 = lax.axis_index("m3"), lax.axis_index("m2"), lax.axis_index("m1")
    n_a, n_b, n_l, _ = x_hbm.shape
    n_ab = n_a // AG
    n_p = n_b // PB
    n_slab = n_ab * n_p
    n_g = grp.shape[0] // 2
    n_t = n_g * n_ab
    n_k = xrecv.shape[2]
    n_j = u2send.shape[2]
    k_part = n_k // n_ab

    def slab_copy(i):
        return pltpu.make_async_copy(
            x_hbm.at[pl.ds(i // n_p * AG, AG), pl.ds(i % n_p * PB, PB)],
            slab.at[i % SLAB_RING], slab_sem.at[i % SLAB_RING])

    def remote(axis, src, dst, send_sem, recv_sem):
        return pltpu.make_async_remote_copy(
            src_ref=src, dst_ref=dst, send_sem=send_sem, recv_sem=recv_sem,
            device_id={axis: 1 - lax.axis_index(axis)}, device_id_type=MESH)

    def y_copy(q):
        t, p = q // n_p, q % n_p
        return remote("m3", grp.at[(1 - m3) * n_g + t // n_ab, t % n_ab, pl.ds(p * PB, PB)],
                      yrecv.at[t // n_ab, t % n_ab, pl.ds(p * PB, PB)], ysend_sem, yrecv_sem.at[q % Y_RING])

    def y_all():
        return remote("m3", grp.at[pl.ds((1 - m3) * n_g, n_g)], yrecv, ysend_sem, yrecv_sem.at[0])

    def x_copy(t, p):
        return remote("m2", u3send.at[t % X_RING, p], xrecv.at[t, p],
                      xsend_sem.at[t % X_RING], xrecv_sem.at[t % X_RING])

    def x_all(t):
        return remote("m2", u3send.at[t % X_RING], xrecv.at[t],
                      xsend_sem.at[t % X_RING], xrecv_sem.at[t % X_RING])

    def c_copy(t):
        g = t // n_ab
        return remote("m1", u2send.at[t % C_RING], w_ref.at[g * SG + n_ab + t % n_ab],
                      csend_sem.at[t % C_RING], crecv_sem.at[g % CG_RING])

    def c_group(g):
        here = w_ref.at[pl.ds(g * SG + n_ab, n_ab)]
        return remote("m1", here, here, csend_sem.at[0], crecv_sem.at[g % CG_RING])

    for i in range(FIRST):
        slab_copy(i).start()
    facs = [pltpu.make_async_copy(src, dst, fac_sem.at[i]) for i, (src, dst) in enumerate(
        ((a3_hbm, a3_ref), (a2_hbm, a2_ref), (a1_hbm, a1_ref), (d_hbm, d_ref)))]
    for fac in facs:
        fac.start()

    barrier = pltpu.get_barrier_semaphore()
    for partner in ({"m3": 1 - m3}, {"m2": 1 - m2}, {"m1": 1 - m1}):
        pl.semaphore_signal(barrier, inc=1, device_id=partner, device_id_type=MESH)

    def regroup(i):
        ab, p = i // n_p, i % n_p
        def one_b(b, carry):
            tiles = skew([slab[i % SLAB_RING, a, b] for a in range(AG)], SG)
            for g in range(2 * n_g):
                grp[g, ab, p * PB + b] = tiles[g]
            return carry

        lax.fori_loop(0, PB, one_b, 0, unroll=8)

        @pl.when(i + SLAB_RING < n_slab)
        def _():
            slab_copy(i + SLAB_RING).start()

    slab_copy(0).wait()
    for i in range(FIRST, SLAB_RING):
        slab_copy(i).start()
    regroup(0)
    pl.semaphore_wait(barrier, 3)
    y_copy(0).start()

    def next_piece(i):
        @pl.when(i < n_slab)
        def _():
            slab_copy(i).wait()
            regroup(i)
        y_copy(i).start()

    each(AHEAD - 1, lambda i: next_piece(i + 1))

    for fac in facs:
        fac.wait()

    k_all, l_all = a3_ref.shape
    rows = k_all * 8
    cols = 2 * 8 * n_l
    r, c = iota((rows, k_all), 0), iota((rows, k_all), 1)
    pick_k = one_hot((r // 8 + m2 * n_k) % k_all == c)
    r, c = iota((l_all, cols), 0), iota((l_all, cols), 1)
    pick_l = one_hot((c // (8 * n_l) + m3) % 2 * n_l + c % n_l == r)
    wide = dot(dot(pick_k, a3_ref[...]).astype(BF16), pick_l)
    r, c = iota((rows, cols), 0), iota((rows, cols), 1)
    l3_ref[...] = jnp.where(r % 8 == c // n_l % 8, wide, 0.0).astype(BF16)

    def order_two():
        size = a2_ref.shape[0]
        r, c = iota((size, size), 0), iota((size, size), 1)
        pick_j = one_hot((r + m1 * n_j) % size == c)
        pick_b = one_hot((c + m2 * n_b) % size == r)
        a2p_ref[...] = dot(dot(pick_j, a2_ref[...]).astype(BF16), pick_b).astype(BF16)

    def order_one(g):
        size = a1_ref.shape[0]
        r, c = iota((size, size), 0), iota((size, size), 1)
        v = r % (2 * n_ab)
        in_block = (r // (2 * n_ab) + 2 * n_g - (m3 * n_g + g)) % AG
        pick_a = one_hot((v // n_ab + m1) % 2 * n_a + v % n_ab * AG + in_block == c)
        a1p_ref[g] = lax.dot_general(pick_a, a1_ref[...], (((1,), (1,)), ((), ())),
                                     preferred_element_type=F32).astype(BF16)

    def mode_three(t, p):
        g, ab, rows = t // n_ab, t % n_ab, pl.ds(p * PB, PB)
        own = grp[m3 * n_g + g, ab, rows].reshape(PB * n_l, LANES)
        got = yrecv[g, ab, rows].reshape(PB * n_l, LANES)
        out = dot(l3_ref[...], jnp.concatenate([own, got], axis=0))
        out = out.reshape(2 * n_k, PB, LANES).astype(BF16)
        u3send[t % X_RING, p] = out[n_k:]
        u3keep[t % 2, p] = out[:n_k]

    def mode_two(t):
        g, ab = t // n_ab, t % n_ab
        for kp in range(0, n_k, 2):
            cols = []
            for k in (kp, kp + 1):
                cols.append(jnp.concatenate([u3keep[t % 2, :, k].reshape(n_b, LANES),
                                             xrecv[t, :, k].reshape(n_b, LANES)], axis=0))
            out = dot(a2p_ref[...], jnp.concatenate(cols, axis=1)).astype(BF16)
            for h in range(2):
                half = out[:, h * LANES:(h + 1) * LANES]
                u2send[t % C_RING, kp + h] = half[n_j:]
                w_ref[g * SG + ab, kp + h] = half[:n_j]
        c_copy(t).start()

    def mode_one(n):
        g, part = n // n_ab, n % n_ab
        here = w_ref.at[pl.ds(g * SG, SG)]
        mode_one_part(here, here, a1p_ref[g], d_ref, part * k_part, part * k_part, k_part)

    def step(t, carry):
        @pl.when((t >= X_RING) & (t < n_t))
        def _():
            x_all(t - X_RING).wait_send()

        def piece(p):
            q = t * n_p + p
            y_copy(q).wait_recv()
            mode_three(t, p)
            x_copy(t, p).start()

            @pl.when(q + AHEAD < n_t * n_p)
            def _():
                next_piece(q + AHEAD)

        @pl.when(t < n_t)
        def _():
            each(n_p, piece)

        @pl.when(t == 0)
        def _():
            order_two()

        u = t - 1

        @pl.when(u >= 0)
        def _():
            x_all(u).wait_recv()

            @pl.when(u >= C_RING)
            def _():
                c_copy(u - C_RING).wait_send()
            mode_two(u)

        @pl.when(t < n_g)
        def _():
            order_one(t)

        n = t - n_ab - 1

        @pl.when(n >= 0)
        def _():
            @pl.when(n % n_ab == 0)
            def _():
                c_group(n // n_ab).wait_recv()
            mode_one(n)
        return carry

    lax.fori_loop(0, n_t + 1, step, 0)

    y_all().wait_send()
    each(X_RING, lambda i: x_all(n_t - X_RING + i).wait_send())
    each(C_RING, lambda i: c_copy(n_t - C_RING + i).wait_send())
    c_group(n_g - 1).wait_recv()


def finish(w_vmem, a1p_ref, d_ref, w_hbm, wst, w_sem, last_sem):
    n_g = w_vmem.shape[0] // SG
    n_k = w_vmem.shape[1]
    parts = wst.shape[0]
    k_part = n_k // parts

    def group_copy(g):
        here = pl.ds(g * SG, SG)
        return pltpu.make_async_copy(w_vmem.at[here], w_hbm.at[here], w_sem)

    def part_copy(i):
        return pltpu.make_async_copy(
            wst.at[i], w_hbm.at[pl.ds((n_g - 1) * SG, SG), pl.ds(i * k_part, k_part)], last_sem)

    each(n_g - 1, lambda g: group_copy(g).start())
    a1p = a1p_ref[n_g - 1]

    def part(i):
        mode_one_part(w_vmem.at[pl.ds((n_g - 1) * SG, SG)], wst.at[i], a1p, d_ref, i * k_part, 0, k_part)
        part_copy(i).start()
    each(parts, part)
    most = pl.ds(0, (n_g - 1) * SG)
    pltpu.make_async_copy(w_vmem.at[most], w_hbm.at[most], w_sem).wait()
    last = pl.ds((n_g - 1) * SG, SG)
    pltpu.make_async_copy(w_vmem.at[last], w_hbm.at[last], last_sem).wait()


def solution(mesh):
    def local_step(vol_blk, fac_one, fac_two, fac_three, diag_blk):
        n_s, n_a, n_b, n_l = vol_blk.shape
        n_k, n_j, n_i = diag_blk.shape
        x = jnp.transpose(vol_blk, (1, 2, 3, 0))
        n_g = n_s // SG // 2
        n_ab = n_a // AG
        n_t = n_g * n_ab
        n_p = n_b // PB
        vmem = pl.BlockSpec(memory_space=pltpu.VMEM)
        dma = pltpu.SemaphoreType.DMA
        w_vmem, a1p, diag = pl.pallas_call(
            kernel,
            out_shape=(pltpu.VMEM((n_s // 2, n_k, n_j, n_i), BF16), pltpu.VMEM((n_g,) + fac_one.shape, BF16),
                       pltpu.VMEM(diag_blk.shape, F32)),
            in_specs=[pl.BlockSpec(memory_space=pl.ANY)] * 5,
            out_specs=(vmem, vmem, vmem),
            scratch_shapes=[
                pltpu.VMEM((SLAB_RING, AG, PB, n_l, LANES), BF16),
                pltpu.VMEM((2 * n_g, n_ab, n_b, n_l, LANES), BF16),
                pltpu.VMEM((n_g, n_ab, n_b, n_l, LANES), BF16),
                pltpu.VMEM((2, n_p, n_k, PB, LANES), BF16),
                pltpu.VMEM((X_RING, n_p, n_k, PB, LANES), BF16),
                pltpu.VMEM((n_t, n_p, n_k, PB, LANES), BF16),
                pltpu.VMEM((C_RING, n_k, n_j, LANES), BF16),
                pltpu.VMEM(fac_one.shape, BF16),
                pltpu.VMEM(fac_two.shape, BF16),
                pltpu.VMEM(fac_three.shape, BF16),
                pltpu.VMEM((fac_three.shape[0] * 8, 2 * 8 * n_l), BF16),
                pltpu.VMEM(fac_two.shape, BF16),
                dma((4,)), dma((SLAB_RING,)),
                dma, dma((Y_RING,)),
                dma((X_RING,)), dma((X_RING,)),
                dma((C_RING,)), dma((CG_RING,)),
            ],
            compiler_params=pltpu.CompilerParams(
                collective_id=0, has_side_effects=True, vmem_limit_bytes=43 * 1024 * 1024),
        )(x, fac_one, fac_two, fac_three, diag_blk)
        return pl.pallas_call(
            finish,
            out_shape=jax.ShapeDtypeStruct(w_vmem.shape, BF16),
            in_specs=[vmem, vmem, vmem],
            out_specs=pl.BlockSpec(memory_space=pl.ANY),
            scratch_shapes=[pltpu.VMEM((n_ab, SG, n_k // n_ab, n_j, n_i), BF16), dma, dma],
            compiler_params=pltpu.CompilerParams(vmem_limit_bytes=8 * 1024 * 1024),
        )(w_vmem, a1p, diag)

    return jax.shard_map(local_step, mesh=mesh, in_specs=(P("dp", "m1", "m2", "m3"), P(), P(), P(), P("m2", "m1", None)), out_specs=P(("dp", "m3"), "m2", "m1", None), check_vma=False)
```

```python
import jax
import jax.numpy as jnp
from jax import lax
from jax.experimental import pallas as pl
from jax.experimental.pallas import tpu as pltpu
from jax.sharding import PartitionSpec as P

MESH = pl.DeviceIdType.MESH
F32, BF16 = jnp.float32, jnp.bfloat16

LANES = 128
SG = 8
AG = 16
PB = 8
SLAB_RING = 4
FIRST = 4
HEAD = 4
AHEAD = 7
Y_RING = 14
X_RING = 4
C_RING = 2
CG_RING = 3


def skew(tiles, step):
    count = len(tiles)
    axis = tiles[0].ndim - 1
    block = lax.broadcasted_iota(jnp.int32, tiles[0].shape, axis) // step
    tiles = [t if i == 0 else pltpu.roll(t, i * step, axis) for i, t in enumerate(tiles)]
    dist = 1
    while dist < count:
        on = (block & dist) != 0
        tiles = [jnp.where(on, tiles[(h + dist) % count], tiles[h]) for h in range(count)]
        dist *= 2
    return [tiles[(count - g) % count] for g in range(count)]


def exchange(tiles, step):
    axis = tiles[0].ndim - 1
    return [t if g == 0 else pltpu.roll(t, LANES - g * step, axis) for g, t in enumerate(skew(tiles, step))]


def iota(shape, axis):
    return lax.broadcasted_iota(jnp.int32, shape, axis)


def one_hot(cond):
    return jnp.where(cond, 1.0, 0.0).astype(BF16)


def dot(a, b):
    return jnp.dot(a, b, preferred_element_type=F32)


def each(count, do):
    def body(i, carry):
        do(i)
        return carry
    lax.fori_loop(0, count, body, 0)


def mode_one_part(src, dst, a1p, d_ref, k_src, k_dst, count):
    n_jt = d_ref.shape[1] // 16

    def body(i, carry):
        k, rows = i // n_jt, pl.ds(i % n_jt * 16, 16)
        tiles = exchange([src[v, k_src + k, rows] for v in range(SG)], 1)
        out = dot(jnp.concatenate(tiles, axis=0), a1p).astype(BF16).astype(F32)
        out = out.reshape(SG, 16, LANES) * d_ref[k_src + k, rows, :][None]
        dst[:, k_dst + k, rows, :] = out.astype(BF16)
        return carry

    lax.fori_loop(0, count * n_jt, body, 0, unroll=count * n_jt)


def kernel(x_hbm, a1_hbm, a2_hbm, a3_hbm, d_hbm, w_ref, a1p_ref, d_ref,
           slab, grp, yrecv, u3keep, u3send, xrecv, u2send,
           a1_ref, a2_ref, a3_ref, l3_ref, a2p_ref,
           head_sem, fac_sem, slab_sem, ysend_sem, yrecv_sem, xsend_sem, xrecv_sem, csend_sem, crecv_sem):
    m3, m2, m1 = lax.axis_index("m3"), lax.axis_index("m2"), lax.axis_index("m1")
    n_a, n_b, n_l, _ = x_hbm.shape
    n_ab = n_a // AG
    n_p = n_b // PB
    n_slab = n_ab * n_p
    n_g = grp.shape[0] // 2
    n_t = n_g * n_ab
    n_k = xrecv.shape[2]
    n_j = u2send.shape[2]
    k_part = n_k // n_ab

    def slab_copy(i):
        return pltpu.make_async_copy(
            x_hbm.at[pl.ds(i // n_p * AG, AG), pl.ds(i % n_p * PB, PB)],
            slab.at[i % SLAB_RING], slab_sem.at[i % SLAB_RING])

    def remote(axis, src, dst, send_sem, recv_sem):
        return pltpu.make_async_remote_copy(
            src_ref=src, dst_ref=dst, send_sem=send_sem, recv_sem=recv_sem,
            device_id={axis: 1 - lax.axis_index(axis)}, device_id_type=MESH)

    def y_copy(q):
        t, p = q // n_p, q % n_p
        return remote("m3", grp.at[(1 - m3) * n_g + t // n_ab, t % n_ab, pl.ds(p * PB, PB)],
                      yrecv.at[t // n_ab, t % n_ab, pl.ds(p * PB, PB)], ysend_sem, yrecv_sem.at[q % Y_RING])

    def y_all():
        return remote("m3", grp.at[pl.ds((1 - m3) * n_g, n_g)], yrecv, ysend_sem, yrecv_sem.at[0])

    def x_copy(t, p):
        return remote("m2", u3send.at[t % X_RING, p], xrecv.at[t, p],
                      xsend_sem.at[t % X_RING], xrecv_sem.at[t % X_RING])

    def x_all(t):
        return remote("m2", u3send.at[t % X_RING], xrecv.at[t],
                      xsend_sem.at[t % X_RING], xrecv_sem.at[t % X_RING])

    def c_copy(t):
        g = t // n_ab
        return remote("m1", u2send.at[t % C_RING], w_ref.at[g * SG + n_ab + t % n_ab],
                      csend_sem.at[t % C_RING], crecv_sem.at[g % CG_RING])

    def c_group(g):
        here = w_ref.at[pl.ds(g * SG + n_ab, n_ab)]
        return remote("m1", here, here, csend_sem.at[0], crecv_sem.at[g % CG_RING])

    def head_copy(h):
        rows = pl.ds(h * HEAD, HEAD)
        return pltpu.make_async_copy(x_hbm.at[pl.ds(0, AG), rows], slab.at[0, :, rows], head_sem.at[h])

    def head_send(h):
        rows = pl.ds(h * HEAD, HEAD)
        return remote("m3", grp.at[(1 - m3) * n_g, 0, rows], yrecv.at[0, 0, rows], ysend_sem, yrecv_sem.at[0])

    for h in range(PB // HEAD):
        head_copy(h).start()
    for i in range(1, FIRST):
        slab_copy(i).start()
    facs = [pltpu.make_async_copy(src, dst, fac_sem.at[i]) for i, (src, dst) in enumerate(
        ((a3_hbm, a3_ref), (a2_hbm, a2_ref), (a1_hbm, a1_ref), (d_hbm, d_ref)))]
    for fac in facs:
        fac.start()

    barrier = pltpu.get_barrier_semaphore()
    for partner in ({"m3": 1 - m3}, {"m2": 1 - m2}, {"m1": 1 - m1}):
        pl.semaphore_signal(barrier, inc=1, device_id=partner, device_id_type=MESH)

    def regroup(i, b0=0, count=PB):
        ab, p = i // n_p, i % n_p
        def one_b(b, carry):
            b = b0 + b
            tiles = skew([slab[i % SLAB_RING, a, b] for a in range(AG)], SG)
            for g in range(2 * n_g):
                grp[g, ab, p * PB + b] = tiles[g]
            return carry

        lax.fori_loop(0, count, one_b, 0, unroll=count)

        if b0 + count < PB:
            return

        @pl.when(i + SLAB_RING < n_slab)
        def _():
            slab_copy(i + SLAB_RING).start()

    for i in range(FIRST, SLAB_RING):
        slab_copy(i).start()
    for h in range(PB // HEAD):
        head_copy(h).wait()
        regroup(0, h * HEAD, HEAD)
        if h == 0:
            pl.semaphore_wait(barrier, 3)
        head_send(h).start()

    def next_piece(i):
        @pl.when(i < n_slab)
        def _():
            slab_copy(i).wait()
            regroup(i)
        y_copy(i).start()

    each(AHEAD - 1, lambda i: next_piece(i + 1))

    for fac in facs:
        fac.wait()

    k_all, l_all = a3_ref.shape
    rows = k_all * 8
    cols = 2 * 8 * n_l
    r, c = iota((rows, k_all), 0), iota((rows, k_all), 1)
    pick_k = one_hot((r // 8 + m2 * n_k) % k_all == c)
    r, c = iota((l_all, cols), 0), iota((l_all, cols), 1)
    pick_l = one_hot((c // (8 * n_l) + m3) % 2 * n_l + c % n_l == r)
    wide = dot(dot(pick_k, a3_ref[...]).astype(BF16), pick_l)
    r, c = iota((rows, cols), 0), iota((rows, cols), 1)
    l3_ref[...] = jnp.where(r % 8 == c // n_l % 8, wide, 0.0).astype(BF16)

    def order_two():
        size = a2_ref.shape[0]
        r, c = iota((size, size), 0), iota((size, size), 1)
        pick_j = one_hot((r + m1 * n_j) % size == c)
        pick_b = one_hot((c + m2 * n_b) % size == r)
        a2p_ref[...] = dot(dot(pick_j, a2_ref[...]).astype(BF16), pick_b).astype(BF16)

    def order_one(g):
        size = a1_ref.shape[0]
        r, c = iota((size, size), 0), iota((size, size), 1)
        v = r % (2 * n_ab)
        in_block = (r // (2 * n_ab) + 2 * n_g - (m3 * n_g + g)) % AG
        pick_a = one_hot((v // n_ab + m1) % 2 * n_a + v % n_ab * AG + in_block == c)
        a1p_ref[g] = lax.dot_general(pick_a, a1_ref[...], (((1,), (1,)), ((), ())),
                                     preferred_element_type=F32).astype(BF16)

    def mode_three(t, p):
        g, ab, rows = t // n_ab, t % n_ab, pl.ds(p * PB, PB)
        own = grp[m3 * n_g + g, ab, rows].reshape(PB * n_l, LANES)
        got = yrecv[g, ab, rows].reshape(PB * n_l, LANES)
        out = dot(l3_ref[...], jnp.concatenate([own, got], axis=0))
        out = out.reshape(2 * n_k, PB, LANES).astype(BF16)
        u3send[t % X_RING, p] = out[n_k:]
        u3keep[t % 2, p] = out[:n_k]

    def mode_two(t):
        g, ab = t // n_ab, t % n_ab
        for kp in range(0, n_k, 2):
            cols = []
            for k in (kp, kp + 1):
                cols.append(jnp.concatenate([u3keep[t % 2, :, k].reshape(n_b, LANES),
                                             xrecv[t, :, k].reshape(n_b, LANES)], axis=0))
            out = dot(a2p_ref[...], jnp.concatenate(cols, axis=1)).astype(BF16)
            for h in range(2):
                half = out[:, h * LANES:(h + 1) * LANES]
                u2send[t % C_RING, kp + h] = half[n_j:]
                w_ref[g * SG + ab, kp + h] = half[:n_j]
        c_copy(t).start()

    def mode_one(n):
        g, part = n // n_ab, n % n_ab
        here = w_ref.at[pl.ds(g * SG, SG)]
        mode_one_part(here, here, a1p_ref[g], d_ref, part * k_part, part * k_part, k_part)

    def step(t, carry):
        @pl.when((t >= X_RING) & (t < n_t))
        def _():
            x_all(t - X_RING).wait_send()

        def piece(p):
            q = t * n_p + p
            y_copy(q).wait_recv()
            mode_three(t, p)
            x_copy(t, p).start()

            @pl.when(q + AHEAD < n_t * n_p)
            def _():
                next_piece(q + AHEAD)

        @pl.when(t < n_t)
        def _():
            each(n_p, piece)

        @pl.when(t == 0)
        def _():
            order_two()

        u = t - 1

        @pl.when(u >= 0)
        def _():
            x_all(u).wait_recv()

            @pl.when(u >= C_RING)
            def _():
                c_copy(u - C_RING).wait_send()
            mode_two(u)

        @pl.when(t < n_g)
        def _():
            order_one(t)

        n = t - n_ab - 1

        @pl.when(n >= 0)
        def _():
            @pl.when(n % n_ab == 0)
            def _():
                c_group(n // n_ab).wait_recv()
            mode_one(n)
        return carry

    lax.fori_loop(0, n_t + 1, step, 0)

    y_all().wait_send()
    each(X_RING, lambda i: x_all(n_t - X_RING + i).wait_send())
    each(C_RING, lambda i: c_copy(n_t - C_RING + i).wait_send())
    c_group(n_g - 1).wait_recv()


def finish(w_vmem, a1p_ref, d_ref, w_hbm, wst, w_sem, last_sem):
    n_g = w_vmem.shape[0] // SG
    n_k = w_vmem.shape[1]
    parts = wst.shape[0]
    k_part = n_k // parts

    def rhs_copy(i):
        here = pl.ds(i, 1)
        return pltpu.make_async_copy(w_vmem.at[here], w_hbm.at[here], w_sem)

    def part_copy(i):
        return pltpu.make_async_copy(
            wst.at[i], w_hbm.at[pl.ds((n_g - 1) * SG, SG), pl.ds(i * k_part, k_part)], last_sem)

    each((n_g - 1) * SG, lambda i: rhs_copy(i).start())
    a1p = a1p_ref[n_g - 1]

    def part(i):
        mode_one_part(w_vmem.at[pl.ds((n_g - 1) * SG, SG)], wst.at[i], a1p, d_ref, i * k_part, 0, k_part)
        part_copy(i).start()
    each(parts, part)
    most = pl.ds(0, (n_g - 1) * SG)
    pltpu.make_async_copy(w_vmem.at[most], w_hbm.at[most], w_sem).wait()
    last = pl.ds((n_g - 1) * SG, SG)
    pltpu.make_async_copy(w_vmem.at[last], w_hbm.at[last], last_sem).wait()


def solution(mesh):
    def local_step(vol_blk, fac_one, fac_two, fac_three, diag_blk):
        n_s, n_a, n_b, n_l = vol_blk.shape
        n_k, n_j, n_i = diag_blk.shape
        x = jnp.transpose(vol_blk, (1, 2, 3, 0))
        n_g = n_s // SG // 2
        n_ab = n_a // AG
        n_t = n_g * n_ab
        n_p = n_b // PB
        vmem = pl.BlockSpec(memory_space=pltpu.VMEM)
        dma = pltpu.SemaphoreType.DMA
        w_vmem, a1p, diag = pl.pallas_call(
            kernel,
            out_shape=(pltpu.VMEM((n_s // 2, n_k, n_j, n_i), BF16), pltpu.VMEM((n_g,) + fac_one.shape, BF16),
                       pltpu.VMEM(diag_blk.shape, F32)),
            in_specs=[pl.BlockSpec(memory_space=pl.ANY)] * 5,
            out_specs=(vmem, vmem, vmem),
            scratch_shapes=[
                pltpu.VMEM((SLAB_RING, AG, PB, n_l, LANES), BF16),
                pltpu.VMEM((2 * n_g, n_ab, n_b, n_l, LANES), BF16),
                pltpu.VMEM((n_g, n_ab, n_b, n_l, LANES), BF16),
                pltpu.VMEM((2, n_p, n_k, PB, LANES), BF16),
                pltpu.VMEM((X_RING, n_p, n_k, PB, LANES), BF16),
                pltpu.VMEM((n_t, n_p, n_k, PB, LANES), BF16),
                pltpu.VMEM((C_RING, n_k, n_j, LANES), BF16),
                pltpu.VMEM(fac_one.shape, BF16),
                pltpu.VMEM(fac_two.shape, BF16),
                pltpu.VMEM(fac_three.shape, BF16),
                pltpu.VMEM((fac_three.shape[0] * 8, 2 * 8 * n_l), BF16),
                pltpu.VMEM(fac_two.shape, BF16),
                dma((PB // HEAD,)), dma((4,)), dma((SLAB_RING,)),
                dma, dma((Y_RING,)),
                dma((X_RING,)), dma((X_RING,)),
                dma((C_RING,)), dma((CG_RING,)),
            ],
            compiler_params=pltpu.CompilerParams(
                collective_id=0, has_side_effects=True, vmem_limit_bytes=43 * 1024 * 1024),
        )(x, fac_one, fac_two, fac_three, diag_blk)
        return pl.pallas_call(
            finish,
            out_shape=jax.ShapeDtypeStruct(w_vmem.shape, BF16),
            in_specs=[vmem, vmem, vmem],
            out_specs=pl.BlockSpec(memory_space=pl.ANY),
            scratch_shapes=[pltpu.VMEM((n_ab, SG, n_k // n_ab, n_j, n_i), BF16), dma, dma],
            compiler_params=pltpu.CompilerParams(vmem_limit_bytes=8 * 1024 * 1024),
        )(w_vmem, a1p, diag)

    return jax.shard_map(local_step, mesh=mesh, in_specs=(P("dp", "m1", "m2", "m3"), P(), P(), P(), P("m2", "m1", None)), out_specs=P(("dp", "m3"), "m2", "m1", None), check_vma=False)
```

```python
import jax
import jax.numpy as jnp
from jax import lax
from jax.experimental import pallas as pl
from jax.experimental.pallas import tpu as pltpu
from jax.sharding import PartitionSpec as P

MESH = pl.DeviceIdType.MESH
F32, BF16 = jnp.float32, jnp.bfloat16

LANES = 128
SG = 8
AG = 16
PB = 8
SLAB_RING = 4
FIRST = 4
HEAD = 4
AHEAD = 7
Y_RING = 14
X_RING = 4
XS_RING = 2
C_RING = 2
CG_RING = 3


def skew(tiles, step):
    count = len(tiles)
    axis = tiles[0].ndim - 1
    block = lax.broadcasted_iota(jnp.int32, tiles[0].shape, axis) // step
    tiles = [t if i == 0 else pltpu.roll(t, i * step, axis) for i, t in enumerate(tiles)]
    dist = 1
    while dist < count:
        on = (block & dist) != 0
        tiles = [jnp.where(on, tiles[(h + dist) % count], tiles[h]) for h in range(count)]
        dist *= 2
    return [tiles[(count - g) % count] for g in range(count)]


def exchange(tiles, step):
    axis = tiles[0].ndim - 1
    return [t if g == 0 else pltpu.roll(t, LANES - g * step, axis) for g, t in enumerate(skew(tiles, step))]


def iota(shape, axis):
    return lax.broadcasted_iota(jnp.int32, shape, axis)


def one_hot(cond):
    return jnp.where(cond, 1.0, 0.0).astype(BF16)


def dot(a, b):
    return jnp.dot(a, b, preferred_element_type=F32)


def each(count, do):
    def body(i, carry):
        do(i)
        return carry
    lax.fori_loop(0, count, body, 0)


def mode_one_part(src, dst, a1p, d_ref, k_src, k_dst, count):
    n_jt = d_ref.shape[1] // 16

    def body(i, carry):
        k, rows = i // n_jt, pl.ds(i % n_jt * 16, 16)
        tiles = exchange([src[v, k_src + k, rows] for v in range(SG)], 1)
        out = dot(jnp.concatenate(tiles, axis=0), a1p).astype(BF16).astype(F32)
        out = out.reshape(SG, 16, LANES) * d_ref[k_src + k, rows, :][None]
        dst[:, k_dst + k, rows, :] = out.astype(BF16)
        return carry

    lax.fori_loop(0, count * n_jt, body, 0, unroll=count * n_jt)


def kernel(x_hbm, a1_hbm, a2_hbm, a3_hbm, d_hbm, w_ref, a1p_ref, d_ref,
           slab, grp, yrecv, u3keep, u3send, xrecv, u2send,
           a1_ref, a2_ref, a3_ref, l3_ref, a2p_ref,
           head_sem, fac_sem, slab_sem, ysend_sem, yrecv_sem, xsend_sem, xrecv_sem, csend_sem, crecv_sem):
    m3, m2, m1 = lax.axis_index("m3"), lax.axis_index("m2"), lax.axis_index("m1")
    n_a, n_b, n_l, _ = x_hbm.shape
    n_ab = n_a // AG
    n_p = n_b // PB
    n_slab = n_ab * n_p
    n_g = grp.shape[0] // 2
    n_t = n_g * n_ab
    n_k = xrecv.shape[2]
    n_j = u2send.shape[2]
    k_part = n_k // n_ab

    def slab_copy(i):
        return pltpu.make_async_copy(
            x_hbm.at[pl.ds(i // n_p * AG, AG), pl.ds(i % n_p * PB, PB)],
            slab.at[i % SLAB_RING], slab_sem.at[i % SLAB_RING])

    def remote(axis, src, dst, send_sem, recv_sem):
        return pltpu.make_async_remote_copy(
            src_ref=src, dst_ref=dst, send_sem=send_sem, recv_sem=recv_sem,
            device_id={axis: 1 - lax.axis_index(axis)}, device_id_type=MESH)

    def y_copy(q):
        t, p = q // n_p, q % n_p
        return remote("m3", grp.at[(1 - m3) * n_g + t // n_ab, t % n_ab, pl.ds(p * PB, PB)],
                      yrecv.at[t // n_ab, t % n_ab, pl.ds(p * PB, PB)], ysend_sem, yrecv_sem.at[q % Y_RING])

    def y_all():
        return remote("m3", grp.at[pl.ds((1 - m3) * n_g, n_g)], yrecv, ysend_sem, yrecv_sem.at[0])

    def x_copy(t, p):
        return remote("m2", u3send.at[t % XS_RING, p], xrecv.at[t, p],
                      xsend_sem.at[t % XS_RING], xrecv_sem.at[t % X_RING])

    def x_all(t):
        return remote("m2", u3send.at[t % XS_RING], xrecv.at[t],
                      xsend_sem.at[t % XS_RING], xrecv_sem.at[t % X_RING])

    def c_copy(t):
        g = t // n_ab
        return remote("m1", u2send.at[t % C_RING], w_ref.at[g * SG + n_ab + t % n_ab],
                      csend_sem.at[t % C_RING], crecv_sem.at[g % CG_RING])

    def c_group(g):
        here = w_ref.at[pl.ds(g * SG + n_ab, n_ab)]
        return remote("m1", here, here, csend_sem.at[0], crecv_sem.at[g % CG_RING])

    def head_copy(h):
        rows = pl.ds(h * HEAD, HEAD)
        return pltpu.make_async_copy(x_hbm.at[pl.ds(0, AG), rows], slab.at[0, :, rows], head_sem.at[h])

    def head_send(h):
        rows = pl.ds(h * HEAD, HEAD)
        return remote("m3", grp.at[(1 - m3) * n_g, 0, rows], yrecv.at[0, 0, rows], ysend_sem, yrecv_sem.at[0])

    for h in range(PB // HEAD):
        head_copy(h).start()
    for i in range(1, FIRST):
        slab_copy(i).start()
    facs = [pltpu.make_async_copy(src, dst, fac_sem.at[i]) for i, (src, dst) in enumerate(
        ((a3_hbm, a3_ref), (a2_hbm, a2_ref), (a1_hbm, a1_ref), (d_hbm, d_ref)))]
    for fac in facs:
        fac.start()

    barrier = pltpu.get_barrier_semaphore()
    for partner in ({"m3": 1 - m3}, {"m2": 1 - m2}, {"m1": 1 - m1}):
        pl.semaphore_signal(barrier, inc=1, device_id=partner, device_id_type=MESH)

    def regroup(i, b0=0, count=PB):
        ab, p = i // n_p, i % n_p
        def one_b(b, carry):
            b = b0 + b
            tiles = skew([slab[i % SLAB_RING, a, b] for a in range(AG)], SG)
            for g in range(2 * n_g):
                grp[g, ab, p * PB + b] = tiles[g]
            return carry

        lax.fori_loop(0, count, one_b, 0, unroll=count)

        if b0 + count < PB:
            return

        @pl.when(i + SLAB_RING < n_slab)
        def _():
            slab_copy(i + SLAB_RING).start()

    for i in range(FIRST, SLAB_RING):
        slab_copy(i).start()
    for h in range(PB // HEAD):
        head_copy(h).wait()
        regroup(0, h * HEAD, HEAD)
        if h == 0:
            pl.semaphore_wait(barrier, 3)
        if h == 0:
            @pl.when(m1 != 0)
            def _():
                head_send(0).start()
        else:
            @pl.when(m1 == 0)
            def _():
                head_send(0).start()
            head_send(1).start()

    def next_piece(i):
        @pl.when(i < n_slab)
        def _():
            slab_copy(i).wait()
            regroup(i)
        y_copy(i).start()

    each(AHEAD - 1, lambda i: next_piece(i + 1))

    for fac in facs:
        fac.wait()

    k_all, l_all = a3_ref.shape
    rows = k_all * 8
    cols = 2 * 8 * n_l
    r, c = iota((rows, k_all), 0), iota((rows, k_all), 1)
    pick_k = one_hot((r // 8 + m2 * n_k) % k_all == c)
    r, c = iota((l_all, cols), 0), iota((l_all, cols), 1)
    pick_l = one_hot((c // (8 * n_l) + m3) % 2 * n_l + c % n_l == r)
    wide = dot(dot(pick_k, a3_ref[...]).astype(BF16), pick_l)
    r, c = iota((rows, cols), 0), iota((rows, cols), 1)
    l3_ref[...] = jnp.where(r % 8 == c // n_l % 8, wide, 0.0).astype(BF16)

    def order_two():
        size = a2_ref.shape[0]
        r, c = iota((size, size), 0), iota((size, size), 1)
        pick_j = one_hot((r + m1 * n_j) % size == c)
        pick_b = one_hot((c + m2 * n_b) % size == r)
        a2p_ref[...] = dot(dot(pick_j, a2_ref[...]).astype(BF16), pick_b).astype(BF16)

    def order_one(g):
        size = a1_ref.shape[0]
        r, c = iota((size, size), 0), iota((size, size), 1)
        v = r % (2 * n_ab)
        in_block = (r // (2 * n_ab) + 2 * n_g - (m3 * n_g + g)) % AG
        pick_a = one_hot((v // n_ab + m1) % 2 * n_a + v % n_ab * AG + in_block == c)
        a1p_ref[g] = lax.dot_general(pick_a, a1_ref[...], (((1,), (1,)), ((), ())),
                                     preferred_element_type=F32).astype(BF16)

    def mode_three(t, p):
        g, ab, rows = t // n_ab, t % n_ab, pl.ds(p * PB, PB)
        own = grp[m3 * n_g + g, ab, rows].reshape(PB * n_l, LANES)
        got = yrecv[g, ab, rows].reshape(PB * n_l, LANES)
        out = dot(l3_ref[...], jnp.concatenate([own, got], axis=0))
        out = out.reshape(2 * n_k, PB, LANES).astype(BF16)
        u3send[t % XS_RING, p] = out[n_k:]
        u3keep[t % 2, p] = out[:n_k]

    def mode_two(t):
        g, ab = t // n_ab, t % n_ab
        for kp in range(0, n_k, 2):
            cols = []
            for k in (kp, kp + 1):
                cols.append(jnp.concatenate([u3keep[t % 2, :, k].reshape(n_b, LANES),
                                             xrecv[t, :, k].reshape(n_b, LANES)], axis=0))
            out = dot(a2p_ref[...], jnp.concatenate(cols, axis=1)).astype(BF16)
            for h in range(2):
                half = out[:, h * LANES:(h + 1) * LANES]
                u2send[t % C_RING, kp + h] = half[n_j:]
                w_ref[g * SG + ab, kp + h] = half[:n_j]
        c_copy(t).start()

    def mode_one(n):
        g, part = n // n_ab, n % n_ab
        here = w_ref.at[pl.ds(g * SG, SG)]
        mode_one_part(here, here, a1p_ref[g], d_ref, part * k_part, part * k_part, k_part)

    def step(t, carry):
        @pl.when((t >= XS_RING) & (t < n_t))
        def _():
            x_all(t - XS_RING).wait_send()

        def piece(p):
            q = t * n_p + p
            y_copy(q).wait_recv()
            mode_three(t, p)
            x_copy(t, p).start()

            @pl.when(q + AHEAD < n_t * n_p)
            def _():
                next_piece(q + AHEAD)

        @pl.when(t < n_t)
        def _():
            each(n_p, piece)

        @pl.when(t == 0)
        def _():
            order_two()

        u = t - 1

        @pl.when(u >= 0)
        def _():
            x_all(u).wait_recv()

            @pl.when(u >= C_RING)
            def _():
                c_copy(u - C_RING).wait_send()
            mode_two(u)

        @pl.when(t < n_g)
        def _():
            order_one(t)

        n = t - n_ab - 1

        @pl.when(n >= 0)
        def _():
            @pl.when(n % n_ab == 0)
            def _():
                c_group(n // n_ab).wait_recv()
            mode_one(n)
        return carry

    lax.fori_loop(0, n_t + 1, step, 0)

    y_all().wait_send()
    each(XS_RING, lambda i: x_all(n_t - XS_RING + i).wait_send())
    each(C_RING, lambda i: c_copy(n_t - C_RING + i).wait_send())
    c_group(n_g - 1).wait_recv()


def finish(w_vmem, a1p_ref, d_ref, w_hbm, wst, w_sem, last_sem):
    n_g = w_vmem.shape[0] // SG
    n_k = w_vmem.shape[1]
    parts = wst.shape[0]
    k_part = n_k // parts

    def rhs_copy(i):
        here = pl.ds(i, 1)
        return pltpu.make_async_copy(w_vmem.at[here], w_hbm.at[here], w_sem)

    def part_copy(i):
        return pltpu.make_async_copy(
            wst.at[i], w_hbm.at[pl.ds((n_g - 1) * SG, SG), pl.ds(i * k_part, k_part)], last_sem)

    each((n_g - 1) * SG, lambda i: rhs_copy(i).start())
    a1p = a1p_ref[n_g - 1]

    def part(i):
        mode_one_part(w_vmem.at[pl.ds((n_g - 1) * SG, SG)], wst.at[i], a1p, d_ref, i * k_part, 0, k_part)
        part_copy(i).start()
    each(parts, part)
    most = pl.ds(0, (n_g - 1) * SG)
    pltpu.make_async_copy(w_vmem.at[most], w_hbm.at[most], w_sem).wait()
    last = pl.ds((n_g - 1) * SG, SG)
    pltpu.make_async_copy(w_vmem.at[last], w_hbm.at[last], last_sem).wait()


def solution(mesh):
    def local_step(vol_blk, fac_one, fac_two, fac_three, diag_blk):
        n_s, n_a, n_b, n_l = vol_blk.shape
        n_k, n_j, n_i = diag_blk.shape
        x = jnp.transpose(vol_blk, (1, 2, 3, 0))
        n_g = n_s // SG // 2
        n_ab = n_a // AG
        n_t = n_g * n_ab
        n_p = n_b // PB
        vmem = pl.BlockSpec(memory_space=pltpu.VMEM)
        dma = pltpu.SemaphoreType.DMA
        w_vmem, a1p, diag = pl.pallas_call(
            kernel,
            out_shape=(pltpu.VMEM((n_s // 2, n_k, n_j, n_i), BF16), pltpu.VMEM((n_g,) + fac_one.shape, BF16),
                       pltpu.VMEM(diag_blk.shape, F32)),
            in_specs=[pl.BlockSpec(memory_space=pl.ANY)] * 5,
            out_specs=(vmem, vmem, vmem),
            scratch_shapes=[
                pltpu.VMEM((SLAB_RING, AG, PB, n_l, LANES), BF16),
                pltpu.VMEM((2 * n_g, n_ab, n_b, n_l, LANES), BF16),
                pltpu.VMEM((n_g, n_ab, n_b, n_l, LANES), BF16),
                pltpu.VMEM((2, n_p, n_k, PB, LANES), BF16),
                pltpu.VMEM((X_RING, n_p, n_k, PB, LANES), BF16),
                pltpu.VMEM((n_t, n_p, n_k, PB, LANES), BF16),
                pltpu.VMEM((C_RING, n_k, n_j, LANES), BF16),
                pltpu.VMEM(fac_one.shape, BF16),
                pltpu.VMEM(fac_two.shape, BF16),
                pltpu.VMEM(fac_three.shape, BF16),
                pltpu.VMEM((fac_three.shape[0] * 8, 2 * 8 * n_l), BF16),
                pltpu.VMEM(fac_two.shape, BF16),
                dma((PB // HEAD,)), dma((4,)), dma((SLAB_RING,)),
                dma, dma((Y_RING,)),
                dma((XS_RING,)), dma((X_RING,)),
                dma((C_RING,)), dma((CG_RING,)),
            ],
            compiler_params=pltpu.CompilerParams(
                collective_id=0, has_side_effects=True, vmem_limit_bytes=43 * 1024 * 1024),
        )(x, fac_one, fac_two, fac_three, diag_blk)
        return pl.pallas_call(
            finish,
            out_shape=jax.ShapeDtypeStruct(w_vmem.shape, BF16),
            in_specs=[vmem, vmem, vmem],
            out_specs=pl.BlockSpec(memory_space=pl.ANY),
            scratch_shapes=[pltpu.VMEM((n_ab, SG, n_k // n_ab, n_j, n_i), BF16), dma, dma],
            compiler_params=pltpu.CompilerParams(vmem_limit_bytes=8 * 1024 * 1024),
        )(w_vmem, a1p, diag)

    return jax.shard_map(local_step, mesh=mesh, in_specs=(P("dp", "m1", "m2", "m3"), P(), P(), P(), P("m2", "m1", None)), out_specs=P(("dp", "m3"), "m2", "m1", None), check_vma=False)
```

```python
import jax
import jax.numpy as jnp
from jax import lax
from jax.experimental import pallas as pl
from jax.experimental.pallas import tpu as pltpu
from jax.sharding import PartitionSpec as P

MESH = pl.DeviceIdType.MESH
F32, BF16 = jnp.float32, jnp.bfloat16

LANES = 128
SG = 8
AG = 16
PB = 8
SLAB_RING = 4
FIRST = 4
HEAD = 4
AHEAD = 6
Y_RING = 12
X_RING = 4
XS_RING = 2
C_RING = 2
CG_RING = 3


def skew(tiles, step):
    count = len(tiles)
    axis = tiles[0].ndim - 1
    block = lax.broadcasted_iota(jnp.int32, tiles[0].shape, axis) // step
    tiles = [t if i == 0 else pltpu.roll(t, i * step, axis) for i, t in enumerate(tiles)]
    dist = 1
    while dist < count:
        on = (block & dist) != 0
        tiles = [jnp.where(on, tiles[(h + dist) % count], tiles[h]) for h in range(count)]
        dist *= 2
    return [tiles[(count - g) % count] for g in range(count)]


def exchange(tiles, step):
    axis = tiles[0].ndim - 1
    return [t if g == 0 else pltpu.roll(t, LANES - g * step, axis) for g, t in enumerate(skew(tiles, step))]


def iota(shape, axis):
    return lax.broadcasted_iota(jnp.int32, shape, axis)


def one_hot(cond):
    return jnp.where(cond, 1.0, 0.0).astype(BF16)


def dot(a, b):
    return jnp.dot(a, b, preferred_element_type=F32)


def each(count, do):
    def body(i, carry):
        do(i)
        return carry
    lax.fori_loop(0, count, body, 0)


def mode_one_part(src, dst, a1p, d_ref, k_src, k_dst, count):
    n_jt = d_ref.shape[1] // 16

    def body(i, carry):
        k, rows = i // n_jt, pl.ds(i % n_jt * 16, 16)
        tiles = exchange([src[v, k_src + k, rows] for v in range(SG)], 1)
        out = dot(jnp.concatenate(tiles, axis=0), a1p).astype(BF16).astype(F32)
        out = out.reshape(SG, 16, LANES) * d_ref[k_src + k, rows, :][None]
        dst[:, k_dst + k, rows, :] = out.astype(BF16)
        return carry

    lax.fori_loop(0, count * n_jt, body, 0, unroll=count * n_jt)


def kernel(x_hbm, a1_hbm, a2_hbm, a3_hbm, d_hbm, w_ref, a1p_ref, d_ref,
           slab, grp, yrecv, u3keep, u3send, xrecv, u2send,
           a1_ref, a2_ref, a3_ref, l3_ref, a2p_ref,
           head_sem, fac_sem, slab_sem, ysend_sem, yrecv_sem, xsend_sem, xrecv_sem, csend_sem, crecv_sem):
    m3, m2, m1 = lax.axis_index("m3"), lax.axis_index("m2"), lax.axis_index("m1")
    n_a, n_b, n_l, _ = x_hbm.shape
    n_ab = n_a // AG
    n_p = n_b // PB
    n_slab = n_ab * n_p
    n_g = grp.shape[0] // 2
    n_t = n_g * n_ab
    n_k = xrecv.shape[2]
    n_j = u2send.shape[2]
    k_part = n_k // n_ab

    def slab_copy(i):
        return pltpu.make_async_copy(
            x_hbm.at[pl.ds(i // n_p * AG, AG), pl.ds(i % n_p * PB, PB)],
            slab.at[i % SLAB_RING], slab_sem.at[i % SLAB_RING])

    def remote(axis, src, dst, send_sem, recv_sem):
        return pltpu.make_async_remote_copy(
            src_ref=src, dst_ref=dst, send_sem=send_sem, recv_sem=recv_sem,
            device_id={axis: 1 - lax.axis_index(axis)}, device_id_type=MESH)

    def y_copy(q):
        t, p = q // n_p, q % n_p
        return remote("m3", grp.at[(1 - m3) * n_g + t // n_ab, t % n_ab, pl.ds(p * PB, PB)],
                      yrecv.at[t // n_ab, t % n_ab, pl.ds(p * PB, PB)], ysend_sem, yrecv_sem.at[q % Y_RING])

    def y_all():
        return remote("m3", grp.at[pl.ds((1 - m3) * n_g, n_g)], yrecv, ysend_sem, yrecv_sem.at[0])

    def x_copy(t, p):
        return remote("m2", u3send.at[t % XS_RING, p], xrecv.at[t, p],
                      xsend_sem.at[t % XS_RING], xrecv_sem.at[t % X_RING])

    def x_all(t):
        return remote("m2", u3send.at[t % XS_RING], xrecv.at[t],
                      xsend_sem.at[t % XS_RING], xrecv_sem.at[t % X_RING])

    def c_copy(t):
        g = t // n_ab
        return remote("m1", u2send.at[t % C_RING], w_ref.at[g * SG + n_ab + t % n_ab],
                      csend_sem.at[t % C_RING], crecv_sem.at[g % CG_RING])

    def c_group(g):
        here = w_ref.at[pl.ds(g * SG + n_ab, n_ab)]
        return remote("m1", here, here, csend_sem.at[0], crecv_sem.at[g % CG_RING])

    def head_copy(h):
        rows = pl.ds(h * HEAD, HEAD)
        return pltpu.make_async_copy(x_hbm.at[pl.ds(0, AG), rows], slab.at[0, :, rows], head_sem.at[h])

    def head_send(h):
        rows = pl.ds(h * HEAD, HEAD)
        return remote("m3", grp.at[(1 - m3) * n_g, 0, rows], yrecv.at[0, 0, rows], ysend_sem, yrecv_sem.at[0])

    for h in range(PB // HEAD):
        head_copy(h).start()
    for i in range(1, FIRST):
        slab_copy(i).start()
    facs = [pltpu.make_async_copy(src, dst, fac_sem.at[i]) for i, (src, dst) in enumerate(
        ((a3_hbm, a3_ref), (a2_hbm, a2_ref), (a1_hbm, a1_ref), (d_hbm, d_ref)))]
    for fac in facs:
        fac.start()

    barrier = pltpu.get_barrier_semaphore()
    for partner in ({"m3": 1 - m3}, {"m2": 1 - m2}, {"m1": 1 - m1}):
        pl.semaphore_signal(barrier, inc=1, device_id=partner, device_id_type=MESH)

    def regroup(i, b0=0, count=PB):
        ab, p = i // n_p, i % n_p
        def one_b(b, carry):
            b = b0 + b
            tiles = skew([slab[i % SLAB_RING, a, b] for a in range(AG)], SG)
            for g in range(2 * n_g):
                grp[g, ab, p * PB + b] = tiles[g]
            return carry

        lax.fori_loop(0, count, one_b, 0, unroll=count)

        if b0 + count < PB:
            return

        @pl.when(i + SLAB_RING < n_slab)
        def _():
            slab_copy(i + SLAB_RING).start()

    for i in range(FIRST, SLAB_RING):
        slab_copy(i).start()
    for h in range(PB // HEAD):
        head_copy(h).wait()
        regroup(0, h * HEAD, HEAD)
        if h == 0:
            pl.semaphore_wait(barrier, 3)
        if h == 0:
            @pl.when(m1 != 0)
            def _():
                head_send(0).start()
        else:
            @pl.when(m1 == 0)
            def _():
                head_send(0).start()
            head_send(1).start()

    def next_piece(i):
        @pl.when(i < n_slab)
        def _():
            slab_copy(i).wait()
            regroup(i)
        y_copy(i).start()

    each(AHEAD - 1, lambda i: next_piece(i + 1))

    for fac in facs:
        fac.wait()

    k_all, l_all = a3_ref.shape
    rows = k_all * 8
    cols = 2 * 8 * n_l
    r, c = iota((rows, k_all), 0), iota((rows, k_all), 1)
    pick_k = one_hot((r // 8 + m2 * n_k) % k_all == c)
    r, c = iota((l_all, cols), 0), iota((l_all, cols), 1)
    pick_l = one_hot((c // (8 * n_l) + m3) % 2 * n_l + c % n_l == r)
    wide = dot(dot(pick_k, a3_ref[...]).astype(BF16), pick_l)
    r, c = iota((rows, cols), 0), iota((rows, cols), 1)
    l3_ref[...] = jnp.where(r % 8 == c // n_l % 8, wide, 0.0).astype(BF16)

    def order_two():
        size = a2_ref.shape[0]
        r, c = iota((size, size), 0), iota((size, size), 1)
        pick_j = one_hot((r + m1 * n_j) % size == c)
        pick_b = one_hot((c + m2 * n_b) % size == r)
        a2p_ref[...] = dot(dot(pick_j, a2_ref[...]).astype(BF16), pick_b).astype(BF16)

    def order_one(g):
        size = a1_ref.shape[0]
        r, c = iota((size, size), 0), iota((size, size), 1)
        v = r % (2 * n_ab)
        in_block = (r // (2 * n_ab) + 2 * n_g - (m3 * n_g + g)) % AG
        pick_a = one_hot((v // n_ab + m1) % 2 * n_a + v % n_ab * AG + in_block == c)
        a1p_ref[g] = lax.dot_general(pick_a, a1_ref[...], (((1,), (1,)), ((), ())),
                                     preferred_element_type=F32).astype(BF16)

    def mode_three(t, p):
        g, ab, rows = t // n_ab, t % n_ab, pl.ds(p * PB, PB)
        own = grp[m3 * n_g + g, ab, rows].reshape(PB * n_l, LANES)
        got = yrecv[g, ab, rows].reshape(PB * n_l, LANES)
        out = dot(l3_ref[...], jnp.concatenate([own, got], axis=0))
        out = out.reshape(2 * n_k, PB, LANES).astype(BF16)
        u3send[t % XS_RING, p] = out[n_k:]
        u3keep[t % 2, p] = out[:n_k]

    def mode_two(t):
        g, ab = t // n_ab, t % n_ab
        for kp in range(0, n_k, 2):
            cols = []
            for k in (kp, kp + 1):
                cols.append(jnp.concatenate([u3keep[t % 2, :, k].reshape(n_b, LANES),
                                             xrecv[t, :, k].reshape(n_b, LANES)], axis=0))
            out = dot(a2p_ref[...], jnp.concatenate(cols, axis=1)).astype(BF16)
            for h in range(2):
                half = out[:, h * LANES:(h + 1) * LANES]
                u2send[t % C_RING, kp + h] = half[n_j:]
                w_ref[g * SG + ab, kp + h] = half[:n_j]
        c_copy(t).start()

    def mode_one(n):
        g, part = n // n_ab, n % n_ab
        here = w_ref.at[pl.ds(g * SG, SG)]
        mode_one_part(here, here, a1p_ref[g], d_ref, part * k_part, part * k_part, k_part)

    def step(t, carry):
        @pl.when((t >= XS_RING) & (t < n_t))
        def _():
            x_all(t - XS_RING).wait_send()

        def piece(p):
            q = t * n_p + p
            y_copy(q).wait_recv()
            mode_three(t, p)
            x_copy(t, p).start()

            @pl.when(q + AHEAD < n_t * n_p)
            def _():
                next_piece(q + AHEAD)

        @pl.when(t < n_t)
        def _():
            each(n_p, piece)

        @pl.when(t == 0)
        def _():
            order_two()

        u = t - 1

        @pl.when(u >= 0)
        def _():
            x_all(u).wait_recv()

            @pl.when(u >= C_RING)
            def _():
                c_copy(u - C_RING).wait_send()
            mode_two(u)

        @pl.when(t < n_g)
        def _():
            order_one(t)

        n = t - n_ab - 1

        @pl.when(n >= 0)
        def _():
            @pl.when(n % n_ab == 0)
            def _():
                c_group(n // n_ab).wait_recv()
            mode_one(n)
        return carry

    lax.fori_loop(0, n_t + 1, step, 0)

    y_all().wait_send()
    each(XS_RING, lambda i: x_all(n_t - XS_RING + i).wait_send())
    each(C_RING, lambda i: c_copy(n_t - C_RING + i).wait_send())
    c_group(n_g - 1).wait_recv()


def finish(w_vmem, a1p_ref, d_ref, w_hbm, wst, w_sem, last_sem):
    n_g = w_vmem.shape[0] // SG
    n_k = w_vmem.shape[1]
    parts = wst.shape[0]
    k_part = n_k // parts

    def rhs_copy(i):
        here = pl.ds(i, 1)
        return pltpu.make_async_copy(w_vmem.at[here], w_hbm.at[here], w_sem)

    def part_copy(i):
        return pltpu.make_async_copy(
            wst.at[i], w_hbm.at[pl.ds((n_g - 1) * SG, SG), pl.ds(i * k_part, k_part)], last_sem)

    each((n_g - 1) * SG, lambda i: rhs_copy(i).start())
    a1p = a1p_ref[n_g - 1]

    def part(i):
        mode_one_part(w_vmem.at[pl.ds((n_g - 1) * SG, SG)], wst.at[i], a1p, d_ref, i * k_part, 0, k_part)
        part_copy(i).start()
    each(parts, part)
    most = pl.ds(0, (n_g - 1) * SG)
    pltpu.make_async_copy(w_vmem.at[most], w_hbm.at[most], w_sem).wait()
    last = pl.ds((n_g - 1) * SG, SG)
    pltpu.make_async_copy(w_vmem.at[last], w_hbm.at[last], last_sem).wait()


def solution(mesh):
    def local_step(vol_blk, fac_one, fac_two, fac_three, diag_blk):
        n_s, n_a, n_b, n_l = vol_blk.shape
        n_k, n_j, n_i = diag_blk.shape
        x = jnp.transpose(vol_blk, (1, 2, 3, 0))
        n_g = n_s // SG // 2
        n_ab = n_a // AG
        n_t = n_g * n_ab
        n_p = n_b // PB
        vmem = pl.BlockSpec(memory_space=pltpu.VMEM)
        dma = pltpu.SemaphoreType.DMA
        w_vmem, a1p, diag = pl.pallas_call(
            kernel,
            out_shape=(pltpu.VMEM((n_s // 2, n_k, n_j, n_i), BF16), pltpu.VMEM((n_g,) + fac_one.shape, BF16),
                       pltpu.VMEM(diag_blk.shape, F32)),
            in_specs=[pl.BlockSpec(memory_space=pl.ANY)] * 5,
            out_specs=(vmem, vmem, vmem),
            scratch_shapes=[
                pltpu.VMEM((SLAB_RING, AG, PB, n_l, LANES), BF16),
                pltpu.VMEM((2 * n_g, n_ab, n_b, n_l, LANES), BF16),
                pltpu.VMEM((n_g, n_ab, n_b, n_l, LANES), BF16),
                pltpu.VMEM((2, n_p, n_k, PB, LANES), BF16),
                pltpu.VMEM((X_RING, n_p, n_k, PB, LANES), BF16),
                pltpu.VMEM((n_t, n_p, n_k, PB, LANES), BF16),
                pltpu.VMEM((C_RING, n_k, n_j, LANES), BF16),
                pltpu.VMEM(fac_one.shape, BF16),
                pltpu.VMEM(fac_two.shape, BF16),
                pltpu.VMEM(fac_three.shape, BF16),
                pltpu.VMEM((fac_three.shape[0] * 8, 2 * 8 * n_l), BF16),
                pltpu.VMEM(fac_two.shape, BF16),
                dma((PB // HEAD,)), dma((4,)), dma((SLAB_RING,)),
                dma, dma((Y_RING,)),
                dma((XS_RING,)), dma((X_RING,)),
                dma((C_RING,)), dma((CG_RING,)),
            ],
            compiler_params=pltpu.CompilerParams(
                collective_id=0, has_side_effects=True, vmem_limit_bytes=43 * 1024 * 1024),
        )(x, fac_one, fac_two, fac_three, diag_blk)
        return pl.pallas_call(
            finish,
            out_shape=jax.ShapeDtypeStruct(w_vmem.shape, BF16),
            in_specs=[vmem, vmem, vmem],
            out_specs=pl.BlockSpec(memory_space=pl.ANY),
            scratch_shapes=[pltpu.VMEM((n_ab, SG, n_k // n_ab, n_j, n_i), BF16), dma, dma],
            compiler_params=pltpu.CompilerParams(vmem_limit_bytes=8 * 1024 * 1024),
        )(w_vmem, a1p, diag)

    return jax.shard_map(local_step, mesh=mesh, in_specs=(P("dp", "m1", "m2", "m3"), P(), P(), P(), P("m2", "m1", None)), out_specs=P(("dp", "m3"), "m2", "m1", None), check_vma=False)
```
